32 devices in a mesh: dp: 8 (over y, x, core), mp: 4 (over z).
Axes of the slice: x: 2, y: 2, z: 4, core: 2. Of those that a mesh axis runs over, the one named last changes fastest.
Arguments:
- acts: bfloat16 [4096, 3072], P('dp'), may hold values from -16 to 16
- grads_out: bfloat16 [4096, 8192], P('dp', 'mp'), may hold values from -0.125 to 0.125
- old_a: float32 [8, 3, 128, 1024], P('dp'), may hold values from -0.09375 to 0.09375
- old_g: float32 [4, 8, 2, 128, 1024], P('mp', 'dp'), may hold values from -0.09375 to 0.09375
- a_inverse: bfloat16 [3072, 1024], P('dp'), may hold values from -0.1875 to 0.1875
- g_inverse: bfloat16 [8192, 1024], P('mp'), may hold values from -0.1875 to 0.1875
- owner_map: int32 [5, 8], replicated, may hold values from 0 to 7, each once within a row
Outputs:
- a_factor: float32 [8, 3, 128, 1024], P('dp')
- g_factor: float32 [4, 8, 2, 128, 1024], P('mp', 'dp')
- preconditioned: bfloat16 [3072, 4, 2048], P(None, 'mp', 'dp')
The draws below stay inside these ranges and needn't reach their ends.
Inputs may be any that keep to these rules, and one draw needn't show every extreme that they name: `owner_map`: each row is a permutation: row k tells, for each of the 8 row strips of factor block k, which dp index holds it. Rows 0 to 2 are the activation blocks, the others the output-gradient blocks of every mp index.
All inputs are finite; a program needn't handle non-finite values.
Results may differ from the reference program's by a relative error of at most 0.02.
Values may be sent and summed in bfloat16 or wider, within the bound.
A program may use at most 128 MiB of HBM per device.

```python
import jax
import jax.numpy as jnp
from jax import lax

D_WIN = 3072
BLOCK = 1024
FF_DEV = 2048
TOK_DEV = 512
TOKENS = 4096
FF_WIN = 8192
NA = 3
NG = 2
STRIP = 128
N_DP = 8
N_MP = 4


def draw_acts(key, part):
    values = jnp.clip(jax.random.normal(jax.random.fold_in(key, 23), (TOKENS, D_WIN), jnp.float32), -5.0, 5.0)
    pairing = jax.random.permutation(jax.random.fold_in(key, 29), N_DP)
    token_block = jnp.arange(TOKENS, dtype=jnp.int32) // TOK_DEV
    feature_block = jnp.arange(D_WIN, dtype=jnp.int32) // (D_WIN // N_DP)
    paired = pairing[token_block][:, None] == feature_block[None, :]
    return jnp.where(paired, 3.0 * values, values).astype(jnp.bfloat16)


def draw_grads_out(key, part):
    spread = TOKENS ** (-0.5)
    values = jnp.clip(jax.random.normal(jax.random.fold_in(key, 37), (TOKENS, FF_WIN), jnp.float32), -6.0, 6.0)
    return (values * spread).astype(jnp.bfloat16)


def levels(own_key, shape, shards, smallest, top_value):
    def one(position, shards_of):
        steps = jax.random.uniform(jax.random.fold_in(jax.random.fold_in(own_key, 6), position), (shards_of,), jnp.float32, smallest / len(shards), top_value / len(shards))
        return jnp.repeat(jnp.exp(steps), shape[position] // shards_of).reshape((-1,) + (1,) * (len(shape) - position - 1))

    loudness = one(*shards[0])
    for cut in shards[1:]:
        loudness = loudness * one(*cut)
    return loudness


def normal_values(key, extent, scale, limit, shards=(), held_as=jnp.bfloat16):
    entries = jax.random.normal(key, extent, jnp.float32) * scale
    if len(shards) > 0:
        entries = levels(key, extent, shards, -0.22, 0.18) * entries
    return jnp.clip(entries, min=-limit, max=limit).astype(held_as)


def setup_inputs(seed: int = 0) -> dict:
    arg_keys = jax.random.split(jax.random.key(seed), 8)
    acts = draw_acts(jax.random.fold_in(arg_keys[7], 71), 0)
    grads_out = draw_grads_out(jax.random.fold_in(arg_keys[7], 71), 0)
    old_a = normal_values(arg_keys[2], (N_DP, NA, STRIP, BLOCK), (TOKENS ** -0.5), 0.09375, ((0, 8),), jnp.float32)
    old_g = normal_values(arg_keys[3], (N_MP, N_DP, NG, STRIP, BLOCK), (TOKENS ** -0.5), 0.09375, ((0, 4), (1, 8)), jnp.float32)
    a_inverse = normal_values(arg_keys[4], (D_WIN, BLOCK), BLOCK ** -0.5, 0.1875, ((0, 8),))
    g_inverse = normal_values(arg_keys[5], (FF_WIN, BLOCK), BLOCK ** -0.5, 0.1875, ((0, 4),))
    owner_map = jax.vmap(lambda own: jax.random.permutation(own, N_DP))(jax.random.split(arg_keys[6], (NA + NG))).reshape((NA + NG, N_DP)).astype(jnp.int32)
    return {"acts": acts, "grads_out": grads_out, "old_a": old_a, "old_g": old_g, "a_inverse": a_inverse, "g_inverse": g_inverse, "owner_map": owner_map}


decay_rate = 0.75


def accumulate(running, pieces):
    act_rows, grad_rows = pieces
    act_blocks = act_rows.reshape(TOK_DEV, NA, BLOCK).astype(jnp.float32)
    grad_blocks = grad_rows.reshape(TOK_DEV, N_MP * NG, BLOCK).astype(jnp.float32)
    act_cov = jnp.einsum('tkb,tkc->kbc', act_blocks, act_blocks) / (TOK_DEV * N_DP)
    grad_cov = jnp.einsum('tkb,tkc->kbc', grad_blocks, grad_blocks)
    partial_grad = jnp.dot(act_rows.T, grad_rows, preferred_element_type=jnp.float32).astype(jnp.bfloat16)
    partial_grad = lax.optimization_barrier(partial_grad).astype(jnp.float32)
    return (running[0] + act_cov, running[1] + grad_cov, running[2] + partial_grad), None


def reference(acts, grads_out, old_a, old_g, a_inverse, g_inverse, owner_map):
    acts_split = acts.reshape(N_DP, TOK_DEV, D_WIN)
    grads_split = grads_out.reshape(N_DP, TOK_DEV, FF_WIN)
    start_state = (jnp.zeros((NA, BLOCK, BLOCK), jnp.float32),
                   jnp.zeros((N_MP * NG, BLOCK, BLOCK), jnp.float32),
                   jnp.zeros((D_WIN, FF_WIN), jnp.float32))
    final, unused = lax.scan(accumulate, start_state, (acts_split, grads_split))
    cov_a = final[0]
    cov_g = final[1]
    grad_sum = final[2]
    owners = jnp.arange(N_DP, dtype=jnp.int32)
    onehot = (owner_map[:, :, None] == owners[None, None, :]).astype(jnp.float32)
    a_strips = cov_a.reshape(NA, N_DP, STRIP, BLOCK)
    a_owned = jnp.einsum('ksd,ksrc->dkrc', onehot[:NA], a_strips, precision=lax.Precision.HIGHEST)
    g_strips = cov_g.reshape(N_MP, NG, N_DP, STRIP, BLOCK)
    g_owned = jnp.einsum('jsd,mjsrc->mdjrc', onehot[NA:], g_strips, precision=lax.Precision.HIGHEST)
    a_factor = decay_rate * old_a + (1.0 - decay_rate) * a_owned
    g_factor = decay_rate * old_g + (1.0 - decay_rate) * g_owned
    grad_low = grad_sum.astype(jnp.bfloat16).astype(jnp.float32)
    g_blocks = g_inverse.reshape(N_MP * NG, BLOCK, BLOCK).astype(jnp.float32)
    right_done = jnp.einsum('rjb,jbc->rjc', grad_low.reshape(D_WIN, N_MP * NG, BLOCK), g_blocks)
    right_done = right_done.astype(jnp.bfloat16).astype(jnp.float32).reshape(NA, BLOCK, FF_WIN)
    a_blocks = a_inverse.reshape(NA, BLOCK, BLOCK).astype(jnp.float32)
    result = jnp.einsum('kbc,kcf->kbf', a_blocks, right_done).astype(jnp.bfloat16)
    return a_factor, g_factor, result.reshape(D_WIN, N_MP, FF_DEV)
```

```python
import functools

import jax
import jax.numpy as jnp
from jax import lax
from jax.experimental import pallas as pl
from jax.experimental.pallas import tpu as pltpu
from jax.sharding import PartitionSpec as P

decay_rate = 0.75
low = jnp.bfloat16
full = jnp.float32


def chip_at(me, slot, order):
    chip = 0
    for place, bit in enumerate(order):
        want = lax.rem(lax.div(jnp.int32(slot), jnp.int32(1 << (len(order) - 1 - place))), jnp.int32(2))
        have = lax.rem(lax.div(me, jnp.int32(1 << bit)), jnp.int32(2))
        chip = chip + (want + have - 2 * want * have) * (1 << bit)
    return chip


def slot_of(relative, order):
    slot = 0
    for place, bit in enumerate(order):
        slot += ((relative >> bit) & 1) << (len(order) - 1 - place)
    return slot


def kernel(
    sizes, owner_map, acts, grads, a_inverse, g_inverse, out, g_cov, a_cov,
    acts2, grads2, g_cols, turned, a_all, flipped, wide, right, out_tile, g_sum, a_rows,
    grad_part, g_part, a_part, grad_came, g_came, a_came, local_sem, send_sem, recv_sem,
):
    dp_count, mp_count, tokens = sizes
    chips = dp_count // 2
    bits = list(range(chips.bit_length() - 1))
    orders = (bits, bits[::-1])
    stages = len(bits)
    own, features = acts.shape
    hidden = grads.shape[1]
    block = a_inverse.shape[1]
    na, ng = features // block, hidden // block
    strip = block // dp_count
    sub = strip // mp_count
    width = hidden // dp_count
    half = block // 2
    shard = a_inverse.shape[0]
    piece = block // mp_count

    dp = lax.axis_index("dp")
    mp = lax.axis_index("mp")
    chip, core = lax.div(dp, jnp.int32(2)), lax.rem(dp, jnp.int32(2))
    partner = (chip * 2 + 1 - core, mp)
    relatives = [chip_at(chip, r, bits[::-1]) for r in range(chips)]
    above = [lax.rem(mp + step, jnp.int32(mp_count)) for step in range(mp_count)]

    sent = []

    def send(src, dst, device):
        place = len(sent)
        copy = pltpu.make_async_remote_copy(
            src_ref=src, dst_ref=dst, send_sem=send_sem.at[place], recv_sem=recv_sem.at[place],
            device_id=device, device_id_type=pl.DeviceIdType.MESH,
        )
        copy.start()
        sent.append(copy)
        return copy

    placed = []

    def move(src, dst):
        copy = pltpu.make_async_copy(src, dst, local_sem.at[len(placed)])
        copy.start()
        placed.append(copy)
        return copy

    def rows_of(chip_index, core_index):
        return pl.ds(pl.multiple_of((chip_index * 2 + core_index) * shard, shard), shard)

    my_piece = pl.ds(pl.multiple_of(mp * piece, piece), piece)

    load_acts = move(acts, acts2.at[:own])
    load_grads = move(grads, grads2.at[:own])
    load_cols = [
        move(
            g_inverse.at[:, pl.ds(pl.multiple_of((2 * u + core) * width, width), width)],
            g_cols.at[:, u * width : (u + 1) * width],
        )
        for u in range(block // width // 2)
    ]
    load_inverse = move(a_inverse, a_all.at[rows_of(chip, core)])

    barrier = pltpu.get_barrier_semaphore()
    peers = [partner]
    peers += [(q * 2 + core, mp) for q in relatives[1:]]
    peers += [(dp, m) for m in above[1:]]
    for peer in peers:
        pl.semaphore_signal(barrier, inc=1, device_id=peer, device_id_type=pl.DeviceIdType.MESH)
    pl.semaphore_wait(barrier, len(peers))

    other_acts = send(acts, acts2.at[own:], partner)
    other_grads = send(grads, grads2.at[own:], partner)
    spread = [
        send(a_inverse.at[:, my_piece], a_all.at[rows_of(chip, core), my_piece], (q * 2 + core, mp))
        for q in relatives[1:]
    ]
    crossed = [send(a_inverse, a_all.at[rows_of(chip, core)], partner)]

    def start(part, came, stage):
        first, last = chips >> (stage + 1), chips >> stage
        copies = []
        for side in range(2):
            bit = orders[side][stage]
            peer = (chip_at(chip, 1 << bit, bits[::-1]) * 2 + core, mp)
            copies.append(send(part.at[side, first:last], came[stage].at[side], peer))
        return copies

    def add(part, came, stage, copies):
        for side in range(2):
            copies[side].wait_recv()
            count = chips >> (stage + 1)

            def one(slot, unused):
                total = part[side, slot].astype(full) + came[stage][side, slot].astype(full)
                part[side, slot] = total.astype(low)
                return unused

            lax.fori_loop(0, count, one, 0)

    def advance(part, came, copies):
        for stage in range(stages - 1):
            add(part, came, stage, copies)
            copies = start(part, came, stage + 1)
        return copies

    def flip_strips(source, block_index, row):
        for r in range(chips):
            owner = relatives[r] * 2 + core
            span = max(strip, 128)
            rows = None
            for start_at in range(0, block, span):
                cols = source[:, pl.ds(pl.multiple_of(block_index * block + start_at, span), span)]
                held = owner_map[row, start_at // strip]
                for inner in range(1, span // strip):
                    held = jnp.where(owner_map[row, start_at // strip + inner] == owner, owner, held)
                rows = cols if rows is None else lax.select(held == owner, cols, rows)
            rows = rows.T
            for inner in range(span // strip):
                part = rows[inner * strip : (inner + 1) * strip]
                if inner == 0:
                    chosen = part
                    continue
                here = jnp.int32(0)
                for s in range(inner, dp_count, span // strip):
                    here = here + jnp.where(owner_map[row, s] == owner, jnp.int32(1), jnp.int32(0))
                chosen = lax.select(here == 1, part, chosen)
            flipped[r * strip : (r + 1) * strip, :] = chosen

    load_acts.wait()
    other_acts.wait_recv()

    def a_block(k, unused):
        flip_strips(acts2, k, k)
        for side in range(2):
            cols = pl.ds(pl.multiple_of(k * block + side * half, half), half)
            wide[...] = jnp.dot(flipped[...], acts2[:, cols], preferred_element_type=full)
            for r in range(chips):
                rows = wide[pl.ds(pl.multiple_of(r * strip + mp * sub, sub), sub), :]
                a_part[side, slot_of(r, orders[side]), k] = (rows / tokens).astype(low)
        return unused

    lax.fori_loop(0, na, a_block, 0)
    a_copies = start(a_part, a_came, 0)

    load_grads.wait()
    other_grads.wait_recv()
    for copy in load_cols:
        copy.wait()

    def turn(j, unused):
        rows = pl.ds(pl.multiple_of(j * block, block), block)
        cols = pl.ds(pl.multiple_of(j * half, half), half)
        turned[:, cols] = jnp.dot(
            grads2[:, rows], g_cols[rows, :], preferred_element_type=full
        ).astype(low)
        return unused

    lax.fori_loop(0, ng, turn, 0)

    def multiply(k):
        for side in range(2):

            def flip_one(v, unused):
                cols = pl.ds(pl.multiple_of(k * block + side * half + v * 128, 128), 128)
                flipped[pl.ds(pl.multiple_of(v * 128, 128), 128), :] = acts2[:, cols].T
                return unused

            lax.fori_loop(0, half // 128, flip_one, 0)

            def product(slot, unused):
                q = chip_at(chip, slot, orders[side])
                cols = pl.ds(pl.multiple_of(q * width, width), width)
                grad_part[k, side, slot] = jnp.dot(
                    flipped[...], turned[:, cols], preferred_element_type=full
                ).astype(low)
                return unused

            lax.fori_loop(0, chips, product, 0)
        return start(grad_part.at[k], [came.at[k] for came in grad_came], 0)

    def advance_grad(k, copies):
        return advance(grad_part.at[k], [came.at[k] for came in grad_came], copies)

    grad_copies = [None] * na
    grad_copies[0] = multiply(0)

    climbed = []
    load_inverse.wait()
    for r in range(1, chips):
        spread[r - 1].wait_recv()
        for m in above[1:]:
            where = a_all.at[rows_of(relatives[r], core), my_piece]
            climbed.append(send(where, where, (dp, m)))

    a_copies = advance(a_part, a_came, a_copies)
    gathered = None
    for k in range(1, na):
        grad_copies[k] = multiply(k)
        grad_copies[k - 1] = advance_grad(k - 1, grad_copies[k - 1])
        if k == 1:
            for side in range(2):
                a_copies[side].wait_recv()
            for side in range(2):
                total = a_part[side, 0].astype(full) + a_came[-1][side, 0].astype(full)
                a_rows[mp, :, :, side * half : (side + 1) * half] = total.astype(low)
            gathered = [send(a_rows.at[mp], a_rows.at[mp], (dp, m)) for m in above[1:]]

    def g_block(j, unused):
        flip_strips(grads2, j, na + j)
        for side in range(2):
            cols = pl.ds(pl.multiple_of(j * block + side * half, half), half)
            wide[...] = jnp.dot(flipped[...], grads2[:, cols], preferred_element_type=full)
            for r in range(chips):
                rows = wide[r * strip : (r + 1) * strip, :]
                g_part[side, slot_of(r, orders[side]), j] = rows.astype(low)
        return unused

    lax.fori_loop(0, ng, g_block, 0)
    g_copies = start(g_part, g_came, 0)
    grad_copies[na - 1] = advance_grad(na - 1, grad_copies[na - 1])

    for r in range(1, chips):
        for step in range(mp_count - 1):
            climbed[(r - 1) * (mp_count - 1) + step].wait_recv()
        where = a_all.at[rows_of(relatives[r], core)]
        crossed.append(send(where, where, partner))

    g_copies = advance(g_part, g_came, g_copies)

    for copy in crossed:
        copy.wait_recv()
    for k in range(na):
        for side in range(2):
            grad_copies[k][side].wait_recv()
            total = grad_part[k, side, 0].astype(full) + grad_came[-1][k, side, 0].astype(full)
            right[side * half : (side + 1) * half, :] = total.astype(low)

        def finish(t, unused):
            rows = pl.ds(pl.multiple_of(k * block + t * 256, 256), 256)
            out_tile[rows, :] = jnp.dot(
                a_all[rows, :], right[...], preferred_element_type=full
            ).astype(low)
            return unused

        lax.fori_loop(0, block // 256, finish, 0)
        done = slice(k * block, (k + 1) * block)
        move(out_tile.at[done], out.at[done])

    for copy in gathered:
        copy.wait_recv()
    move(a_rows, a_cov)
    for side in range(2):
        g_copies[side].wait_recv()
        total = g_part[side, 0].astype(full) + g_came[-1][side, 0].astype(full)
        g_sum[:, :, side * half : (side + 1) * half] = total.astype(low)
    move(g_sum, g_cov)
    for copy in placed[-(na + 2) :]:
        copy.wait()
    for copy in sent:
        copy.wait_send()


def per_device(acts, grads_out, old_a, old_g, a_inverse, g_inverse, owner_map):
    dp_count = lax.axis_size("dp")
    mp_count = lax.axis_size("mp")
    chips = dp_count // 2
    stages = chips.bit_length() - 1
    own, features = acts.shape
    hidden = grads_out.shape[1]
    block = a_inverse.shape[1]
    na, ng = features // block, hidden // block
    strip = block // dp_count
    sub = strip // mp_count
    width = hidden // dp_count
    half = block // 2
    copies = 2 + (chips - 1) * (mp_count + 1) + 1 + (na + 2) * 2 * stages + mp_count - 1
    loads = 3 + block // width // 2 + na + 2

    def came(*shape):
        return [pltpu.VMEM((*shape[0], chips >> (s + 1), *shape[1]), low) for s in range(stages)]

    scratch = [
        pltpu.VMEM((2 * own, features), low),
        pltpu.VMEM((2 * own, hidden), low),
        pltpu.VMEM((hidden, half), low),
        pltpu.VMEM((2 * own, hidden // 2), low),
        pltpu.VMEM((features, block), low),
        pltpu.VMEM((half, 2 * own), low),
        pltpu.VMEM((half, half), full),
        pltpu.VMEM((block, width), low),
        pltpu.VMEM((features, width), low),
        pltpu.VMEM((ng, strip, block), low),
        pltpu.VMEM((mp_count, na, sub, block), low),
        pltpu.VMEM((na, 2, chips, half, width), low),
        pltpu.VMEM((2, chips, ng, strip, half), low),
        pltpu.VMEM((2, chips, na, sub, half), low),
        came((na, 2), (half, width)),
        came((2,), (ng, strip, half)),
        came((2,), (na, sub, half)),
        pltpu.SemaphoreType.DMA((loads,)),
        pltpu.SemaphoreType.DMA((copies,)),
        pltpu.SemaphoreType.DMA((copies,)),
    ]
    anywhere = pl.BlockSpec(memory_space=pl.ANY)
    out, g_cov, a_cov = pl.pallas_call(
        functools.partial(kernel, (dp_count, mp_count, own * dp_count)),
        out_shape=(
            jax.ShapeDtypeStruct((features, width), low),
            jax.ShapeDtypeStruct((ng, strip, block), low),
            jax.ShapeDtypeStruct((mp_count, na, sub, block), low),
        ),
        in_specs=[pl.BlockSpec(memory_space=pltpu.SMEM)] + [anywhere] * 4,
        out_specs=(anywhere,) * 3,
        scratch_shapes=scratch,
        compiler_params=pltpu.CompilerParams(
            collective_id=0, has_side_effects=True, vmem_limit_bytes=60 * 1024 * 1024
        ),
        name="step",
    )(owner_map, acts, grads_out, a_inverse, g_inverse)
    a_cov = a_cov.transpose(1, 0, 2, 3).reshape(old_a.shape).astype(full)
    g_cov = g_cov.reshape(old_g.shape).astype(full)
    a_factor = decay_rate * old_a + (1.0 - decay_rate) * a_cov
    g_factor = decay_rate * old_g + (1.0 - decay_rate) * g_cov
    return (a_factor, g_factor, out.reshape(features, 1, width))


def solution(mesh):
    placed = (
        P("dp", None),
        P("dp", "mp"),
        P("dp", None, None, None),
        P("mp", "dp", None, None, None),
        P("dp", None),
        P("mp", None),
        P(),
    )
    return jax.shard_map(
        per_device,
        mesh=mesh,
        in_specs=placed,
        out_specs=(P("dp", None, None, None), P("mp", "dp", None, None, None), P(None, "mp", "dp")),
        check_vma=False,
    )
```

```python
import functools

import jax
import jax.numpy as jnp
from jax import lax
from jax.experimental import pallas as pl
from jax.experimental.pallas import tpu as pltpu
from jax.sharding import PartitionSpec as P

decay_rate = 0.75
low = jnp.bfloat16
full = jnp.float32


def chip_at(me, slot, order):
    chip = 0
    for place, bit in enumerate(order):
        want = lax.rem(lax.div(jnp.int32(slot), jnp.int32(1 << (len(order) - 1 - place))), jnp.int32(2))
        have = lax.rem(lax.div(me, jnp.int32(1 << bit)), jnp.int32(2))
        chip = chip + (want + have - 2 * want * have) * (1 << bit)
    return chip


def slot_of(relative, order):
    slot = 0
    for place, bit in enumerate(order):
        slot += ((relative >> bit) & 1) << (len(order) - 1 - place)
    return slot


def kernel(
    sizes, owner_map, acts, grads, a_inverse, g_inverse, old_a, old_g, out_tile, a_new, g_new,
    acts2, grads2, g_cols, turned, a_all, flipped, wide, right, a_rows, a_old, g_old,
    grad_part, g_part, a_part, grad_came, g_came, a_came, local_sem, send_sem, recv_sem,
):
    dp_count, mp_count, tokens = sizes
    chips = dp_count // 2
    bits = list(range(chips.bit_length() - 1))
    orders = (bits, bits[::-1])
    stages = len(bits)
    own, features = acts.shape
    hidden = grads.shape[1]
    block = a_inverse.shape[1]
    na, ng = features // block, hidden // block
    strip = block // dp_count
    sub = strip // mp_count
    width = hidden // dp_count
    half = block // 2
    shard = a_inverse.shape[0]
    piece = block // mp_count

    dp = lax.axis_index("dp")
    mp = lax.axis_index("mp")
    chip, core = lax.div(dp, jnp.int32(2)), lax.rem(dp, jnp.int32(2))
    partner = (chip * 2 + 1 - core, mp)
    relatives = [chip_at(chip, r, bits[::-1]) for r in range(chips)]
    above = [lax.rem(mp + step, jnp.int32(mp_count)) for step in range(mp_count)]

    sent = []

    def send(src, dst, device):
        place = len(sent)
        copy = pltpu.make_async_remote_copy(
            src_ref=src, dst_ref=dst, send_sem=send_sem.at[place], recv_sem=recv_sem.at[place],
            device_id=device, device_id_type=pl.DeviceIdType.MESH,
        )
        copy.start()
        sent.append(copy)
        return copy

    placed = []

    def move(src, dst):
        copy = pltpu.make_async_copy(src, dst, local_sem.at[len(placed)])
        copy.start()
        placed.append(copy)
        return copy

    def rows_of(chip_index, core_index, part=None):
        first = (chip_index * 2 + core_index) * shard
        if part is None:
            return pl.ds(pl.multiple_of(first, shard), shard)
        return pl.ds(pl.multiple_of(first + part * (shard // 2), shard // 2), shard // 2)

    my_piece = pl.ds(pl.multiple_of(mp * piece, piece), piece)

    load_inverse = move(a_inverse, a_all.at[rows_of(chip, core)])
    load_grads = move(grads, grads2.at[:own])
    load_cols = [
        move(
            g_inverse.at[:, pl.ds(pl.multiple_of((2 * u + core) * width, width), width)],
            g_cols.at[:, u * width : (u + 1) * width],
        )
        for u in range(block // width // 2)
    ]
    load_acts = move(acts, acts2.at[:own])
    load_old_a = move(old_a.at[0], a_old)
    load_old_g = move(old_g.at[0, 0], g_old)

    with jax.named_scope("barrier"):
        barrier = pltpu.get_barrier_semaphore()
        peers = [partner]
        peers += [(q * 2 + core, mp) for q in relatives[1:]]
        peers += [(dp, m) for m in above[1:]]
        for peer in peers:
            pl.semaphore_signal(barrier, inc=1, device_id=peer, device_id_type=pl.DeviceIdType.MESH)
        pl.semaphore_wait(barrier, len(peers))

    other_grads = send(grads, grads2.at[own:], partner)
    other_acts = [
        send(acts.at[:, i * half : (i + 1) * half], acts2.at[own:, i * half : (i + 1) * half], partner)
        for i in range(2 * na)
    ]

    spread = {}
    waited = set()

    def pass_on(stage, relative):
        for side in range(2):
            order = orders[side]
            held = sum(((relative >> i) & 1) << order[i] for i in range(stage))
            peer = (relatives[1 << order[stage]] * 2 + core, mp)
            where = (rows_of(relatives[held], core, side), my_piece)
            if held:
                spread[side, held].wait_recv()
                waited.add((side, held))
            spread[side, held | (1 << order[stage])] = send(a_all.at[where], a_all.at[where], peer)

    load_inverse.wait()
    for stage in range(stages):
        pass_on(stage, 0)
    crossed = [send(a_inverse, a_all.at[rows_of(chip, core)], partner)]

    def start_side(part, came, stage, side):
        first, last = chips >> (stage + 1), chips >> stage
        peer = (relatives[1 << orders[side][stage]] * 2 + core, mp)
        return send(part.at[side, first:last], came[stage].at[side], peer)

    def start(part, came, stage):
        return [start_side(part, came, stage, side) for side in range(2)]

    def add(part, came, stage, copies):
        for side in range(2):
            copies[side].wait_recv()
            count = chips >> (stage + 1)

            def one(slot, unused):
                total = part[side, slot].astype(full) + came[stage][side, slot].astype(full)
                part[side, slot] = total.astype(low)
                return unused

            lax.fori_loop(0, count, one, 0)

    def advance(part, came, copies):
        for stage in range(stages - 1):
            add(part, came, stage, copies)
            copies = start(part, came, stage + 1)
        return copies

    def flip_strips(source, block_index, row):
        for r in range(chips):
            owner = relatives[r] * 2 + core
            span = max(strip, 128)
            rows = None
            for start_at in range(0, block, span):
                cols = source[:, pl.ds(pl.multiple_of(block_index * block + start_at, span), span)]
                held = owner_map[row, start_at // strip]
                for inner in range(1, span // strip):
                    held = jnp.where(owner_map[row, start_at // strip + inner] == owner, owner, held)
                rows = cols if rows is None else lax.select(held == owner, cols, rows)
            rows = rows.T
            for inner in range(span // strip):
                part = rows[inner * strip : (inner + 1) * strip]
                if inner == 0:
                    chosen = part
                    continue
                here = jnp.int32(0)
                for s in range(inner, dp_count, span // strip):
                    here = here + jnp.where(owner_map[row, s] == owner, jnp.int32(1), jnp.int32(0))
                chosen = lax.select(here == 1, part, chosen)
            flipped[0, r * strip : (r + 1) * strip, :] = chosen

    def turn(first):
        def one(j, unused):
            rows = pl.ds(pl.multiple_of(j * block, block), block)
            cols = pl.ds(pl.multiple_of(j * half, half), half)
            turned[first : first + own, cols] = jnp.dot(
                grads2[first : first + own, rows], g_cols[rows, :], preferred_element_type=full
            ).astype(low)
            return unused

        lax.fori_loop(0, ng, one, 0)

    with jax.named_scope("turn_own"):
        load_grads.wait()
        for copy in load_cols:
            copy.wait()
        turn(0)
    with jax.named_scope("pass_on"):
        for stage in range(1, stages):
            for relative in range(1, 1 << stage):
                pass_on(stage, relative)
    with jax.named_scope("turn_other"):
        other_grads.wait_recv()
        turn(own)

    def multiply(k):
        part = grad_part.at[k]
        came = [came.at[k] for came in grad_came]
        copies = []
        for first, last in ((chips // 2, chips), (0, chips // 2)):
            for side in range(2):
                if first:
                    if k < 2:
                        other_acts[2 * k + side].wait_recv()

                    def flip_one(v, unused):
                        cols = pl.ds(pl.multiple_of(k * block + side * half + v * 128, 128), 128)
                        rows = pl.ds(pl.multiple_of(v * 128, 128), 128)
                        flipped[side, rows, :] = acts2[:, cols].T
                        return unused

                    lax.fori_loop(0, half // 128, flip_one, 0)

                def product(slot, unused):
                    q = chip_at(chip, slot, orders[side])
                    cols = pl.ds(pl.multiple_of(q * width, width), width)
                    part[side, slot] = jnp.dot(
                        flipped[side], turned[:, cols], preferred_element_type=full
                    ).astype(low)
                    return unused

                lax.fori_loop(first, last, product, 0)
                if first:
                    copies.append(start_side(part, came, 0, side))
        return copies

    def advance_grad(k, copies):
        return advance(grad_part.at[k], [came.at[k] for came in grad_came], copies)

    def a_block(k, unused):
        flip_strips(acts2, k, k)
        for side in range(2):
            cols = pl.ds(pl.multiple_of(k * block + side * half, half), half)
            wide[...] = jnp.dot(flipped[0], acts2[:, cols], preferred_element_type=full)
            for r in range(chips):
                rows = wide[pl.ds(pl.multiple_of(r * strip + mp * sub, sub), sub), :]
                a_part[side, slot_of(r, orders[side]), k] = (rows / tokens).astype(low)
        return unused

    with jax.named_scope("wait_acts"):
        load_acts.wait()
    grad_copies = [None] * na
    with jax.named_scope("multiply0"):
        grad_copies[0] = multiply(0)

    with jax.named_scope("climb"):
        climbed = []
        for r in range(1, chips):
            for side in range(2):
                if (side, r) not in waited:
                    spread[side, r].wait_recv()
            where = a_all.at[rows_of(relatives[r], core), my_piece]
            climbed.append([send(where, where, (dp, m)) for m in above[1:]])

    for k in range(1, na):
        with jax.named_scope(f"multiply{k}"):
            grad_copies[k] = multiply(k)
        if k == 1:
            with jax.named_scope("a_block"):
                for later in range(4, 2 * na):
                    other_acts[later].wait_recv()
                lax.fori_loop(0, na, a_block, 0)
                a_copies = start(a_part, a_came, 0)
        if k == na - 1:
            with jax.named_scope("advance_a"):
                a_copies = advance(a_part, a_came, a_copies)
        with jax.named_scope(f"advance{k - 1}"):
            grad_copies[k - 1] = advance_grad(k - 1, grad_copies[k - 1])

    def g_block(j, unused):
        flip_strips(grads2, j, na + j)
        for side in range(2):
            cols = pl.ds(pl.multiple_of(j * block + side * half, half), half)
            wide[...] = jnp.dot(flipped[0], grads2[:, cols], preferred_element_type=full)
            for r in range(chips):
                rows = wide[r * strip : (r + 1) * strip, :]
                g_part[side, slot_of(r, orders[side]), j] = rows.astype(low)
        return unused

    with jax.named_scope("g_block"):
        lax.fori_loop(0, ng, g_block, 0)
        g_copies = start(g_part, g_came, 0)
    with jax.named_scope(f"advance{na - 1}"):
        grad_copies[na - 1] = advance_grad(na - 1, grad_copies[na - 1])
    with jax.named_scope("gather_a"):
        for side in range(2):
            a_copies[side].wait_recv()
        for side in range(2):
            total = a_part[side, 0].astype(full) + a_came[-1][side, 0].astype(full)
            a_rows[mp, :, :, side * half : (side + 1) * half] = total.astype(low)
        gathered = [send(a_rows.at[mp], a_rows.at[mp], (dp, m)) for m in above[1:]]

    with jax.named_scope("cross"):
        for r in range(1, chips):
            for copy in climbed[r - 1]:
                copy.wait_recv()
            where = a_all.at[rows_of(relatives[r], core)]
            crossed.append(send(where, where, partner))
    with jax.named_scope("wait_cross"):
        for copy in crossed:
            copy.wait_recv()

    def finish(k):
        for side in range(2):
            grad_copies[k][side].wait_recv()
            total = grad_part[k, side, 0].astype(full) + grad_came[-1][k, side, 0].astype(full)
            right[side * half : (side + 1) * half, :] = total.astype(low)

        def rows_done(t, unused):
            rows = pl.ds(pl.multiple_of(k * block + t * 256, 256), 256)
            out_tile[rows, :] = jnp.dot(
                a_all[rows, :], right[...], preferred_element_type=full
            ).astype(low)
            return unused

        lax.fori_loop(0, block // 256, rows_done, 0)

    for k in range(na - 1):
        with jax.named_scope(f"finish{k}"):
            finish(k)
    with jax.named_scope("advance_g"):
        g_copies = advance(g_part, g_came, g_copies)
    with jax.named_scope(f"finish{na - 1}"):
        finish(na - 1)

    with jax.named_scope("wait_gather"):
        for copy in gathered:
            copy.wait_recv()
    with jax.named_scope("finish_a"):
        load_old_a.wait()
        for m in range(mp_count):
            rows = slice(m * sub, (m + 1) * sub)
            a_new[:, rows, :] = decay_rate * a_old[:, rows, :] + (1.0 - decay_rate) * a_rows[m].astype(full)
    with jax.named_scope("wait_g"):
        for side in range(2):
            g_copies[side].wait_recv()
    with jax.named_scope("finish_g"):
        load_old_g.wait()
        for side in range(2):
            total = g_part[side, 0].astype(full) + g_came[-1][side, 0].astype(full)
            cols = slice(side * half, (side + 1) * half)
            total = total.astype(low).astype(full)
            g_new[:, :, cols] = decay_rate * g_old[:, :, cols] + (1.0 - decay_rate) * total
    for copy in sent:
        copy.wait_send()


def store(*refs):
    count = len(refs) // 2
    copies = [
        pltpu.make_async_copy(refs[i], refs[count + i], refs[-1].at[i]) for i in range(count)
    ]
    for copy in copies:
        copy.start()
    for copy in copies:
        copy.wait()


def per_device(acts, grads_out, old_a, old_g, a_inverse, g_inverse, owner_map):
    dp_count = lax.axis_size("dp")
    mp_count = lax.axis_size("mp")
    chips = dp_count // 2
    stages = chips.bit_length() - 1
    own, features = acts.shape
    hidden = grads_out.shape[1]
    block = a_inverse.shape[1]
    na, ng = features // block, hidden // block
    strip = block // dp_count
    sub = strip // mp_count
    width = hidden // dp_count
    half = block // 2
    copies = 1 + 2 * na + (chips - 1) * (mp_count + 2) + 1 + (na + 2) * 2 * stages + mp_count - 1
    loads = 5 + block // width // 2

    def came(*shape):
        return [pltpu.VMEM((*shape[0], chips >> (s + 1), *shape[1]), low) for s in range(stages)]

    scratch = [
        pltpu.VMEM((2 * own, features), low),
        pltpu.VMEM((2 * own, hidden), low),
        pltpu.VMEM((hidden, half), low),
        pltpu.VMEM((2 * own, hidden // 2), low),
        pltpu.VMEM((features, block), low),
        pltpu.VMEM((2, half, 2 * own), low),
        pltpu.VMEM((half, half), full),
        pltpu.VMEM((block, width), low),
        pltpu.VMEM((mp_count, na, sub, block), low),
        pltpu.VMEM((na, strip, block), full),
        pltpu.VMEM((ng, strip, block), full),
        pltpu.VMEM((na, 2, chips, half, width), low),
        pltpu.VMEM((2, chips, ng, strip, half), low),
        pltpu.VMEM((2, chips, na, sub, half), low),
        came((na, 2), (half, width)),
        came((2,), (ng, strip, half)),
        came((2,), (na, sub, half)),
        pltpu.SemaphoreType.DMA((loads,)),
        pltpu.SemaphoreType.DMA((copies,)),
        pltpu.SemaphoreType.DMA((copies,)),
    ]
    outside = pl.BlockSpec(memory_space=pltpu.HBM)
    out, a_new, g_new = pl.pallas_call(
        functools.partial(kernel, (dp_count, mp_count, own * dp_count)),
        out_shape=(
            pltpu.VMEM((features, width), low),
            pltpu.VMEM((na, strip, block), full),
            pltpu.VMEM((ng, strip, block), full),
        ),
        in_specs=[pl.BlockSpec(memory_space=pltpu.SMEM)] + [outside] * 6,
        out_specs=(pl.BlockSpec(memory_space=pltpu.VMEM),) * 3,
        scratch_shapes=scratch,
        compiler_params=pltpu.CompilerParams(
            collective_id=0, has_side_effects=True, vmem_limit_bytes=59 * 1024 * 1024 + 7 * 1024 * 100
        ),
        name="step",
    )(owner_map, acts, grads_out, a_inverse, g_inverse, old_a, old_g)
    a_new, g_new, out = pl.pallas_call(
        store,
        out_shape=tuple(jax.ShapeDtypeStruct(x.shape, x.dtype) for x in (a_new, g_new, out)),
        in_specs=[pl.BlockSpec(memory_space=pltpu.VMEM)] * 3,
        out_specs=(pl.BlockSpec(memory_space=pl.ANY),) * 3,
        scratch_shapes=[pltpu.SemaphoreType.DMA((3,))],
        compiler_params=pltpu.CompilerParams(vmem_limit_bytes=1024 * 1024),
        name="store",
    )(a_new, g_new, out)
    return (a_new.reshape(old_a.shape), g_new.reshape(old_g.shape), out.reshape(features, 1, width))


def solution(mesh):
    placed = (
        P("dp", None),
        P("dp", "mp"),
        P("dp", None, None, None),
        P("mp", "dp", None, None, None),
        P("dp", None),
        P("mp", None),
        P(),
    )
    return jax.shard_map(
        per_device,
        mesh=mesh,
        in_specs=placed,
        out_specs=(P("dp", None, None, None), P("mp", "dp", None, None, None), P(None, "mp", "dp")),
        check_vma=False,
    )
```

```python
import functools

import jax
import jax.numpy as jnp
from jax import lax
from jax.experimental import pallas as pl
from jax.experimental.pallas import tpu as pltpu
from jax.sharding import PartitionSpec as P

decay_rate = 0.75
low = jnp.bfloat16
full = jnp.float32


def chip_at(me, slot, order):
    chip = 0
    for place, bit in enumerate(order):
        want = lax.rem(lax.div(jnp.int32(slot), jnp.int32(1 << (len(order) - 1 - place))), jnp.int32(2))
        have = lax.rem(lax.div(me, jnp.int32(1 << bit)), jnp.int32(2))
        chip = chip + (want + have - 2 * want * have) * (1 << bit)
    return chip


def slot_of(relative, order):
    slot = 0
    for place, bit in enumerate(order):
        slot += ((relative >> bit) & 1) << (len(order) - 1 - place)
    return slot


def kernel(
    sizes, map_in, acts, grads, a_inverse, g_inverse, old_a, old_g, out_tile, a_new, g_new,
    acts2, grads2, g_cols, turned, a_all, flipped, wide, right, a_rows, g_rows, a_old, g_old,
    owner_map, grad_part, g_part, a_part, grad_came, g_came, a_came, sym, local_sem, send_sem, recv_sem,
):
    dp_count, mp_count, tokens = sizes
    chips = dp_count // 2
    bits = list(range(chips.bit_length() - 1))
    orders = (bits, bits[::-1])
    stages = len(bits)
    own, features = acts.shape
    hidden = grads.shape[1]
    block = a_inverse.shape[1]
    na, ng = features // block, hidden // block
    strip = block // dp_count
    sub = strip // mp_count
    width = hidden // dp_count
    half = block // 2
    shard = a_inverse.shape[0]
    piece = block // mp_count

    dp = lax.axis_index("dp")
    mp = lax.axis_index("mp")
    chip, core = lax.div(dp, jnp.int32(2)), lax.rem(dp, jnp.int32(2))
    partner = (chip * 2 + 1 - core, mp)
    relatives = [chip_at(chip, r, bits[::-1]) for r in range(chips)]
    folded = chips == 4 and ng == 2 and strip % 128 == 0
    above = [lax.rem(mp + step, jnp.int32(mp_count)) for step in range(mp_count)]

    sent = []

    def send(src, dst, device):
        place = len(sent)
        copy = pltpu.make_async_remote_copy(
            src_ref=src, dst_ref=dst, send_sem=send_sem.at[place], recv_sem=recv_sem.at[place],
            device_id=device, device_id_type=pl.DeviceIdType.MESH,
        )
        copy.start()
        sent.append(copy)
        return copy

    placed = []

    def move(src, dst):
        copy = pltpu.make_async_copy(src, dst, local_sem.at[len(placed)])
        copy.start()
        placed.append(copy)
        return copy

    def rows_of(chip_index, core_index, part=None):
        first = (chip_index * 2 + core_index) * shard
        if part is None:
            return pl.ds(pl.multiple_of(first, shard), shard)
        return pl.ds(pl.multiple_of(first + part * (shard // 2), shard // 2), shard // 2)

    my_piece = pl.ds(pl.multiple_of(mp * piece, piece), piece)

    load_inverse = move(a_inverse, a_all.at[rows_of(chip, core)])
    load_grads = move(grads, grads2.at[:own])
    load_cols = [
        move(
            g_inverse.at[:, pl.ds(pl.multiple_of((2 * u + core) * width, width), width)],
            g_cols.at[:, u * width : (u + 1) * width],
        )
        for u in range(block // width // 2)
    ]
    load_acts = move(acts, acts2.at[:own])
    load_map = move(map_in, owner_map)
    load_old_a = move(old_a.at[0], a_old)
    load_old_g = move(old_g.at[0, 0], g_old)

    with jax.named_scope("barrier"):
        barrier = pltpu.get_barrier_semaphore()
        peers = [partner]
        peers += [(q * 2 + core, mp) for q in relatives[1:]]
        peers += [(dp, m) for m in above[1:]]
        for peer in peers:
            pl.semaphore_signal(barrier, inc=1, device_id=peer, device_id_type=pl.DeviceIdType.MESH)
        pl.semaphore_wait(barrier, len(peers))

    other_grads = send(grads, grads2.at[own:], partner)
    other_acts = [
        send(acts.at[:, i * half : (i + 1) * half], acts2.at[own:, i * half : (i + 1) * half], partner)
        for i in range(2 * na)
    ]

    spread = {}
    climbed = {}

    def arrive(side, held):
        if (side, held) not in climbed:
            spread[side, held].wait_recv()

    def climb(side, held):
        if (side, held) not in climbed:
            where = (rows_of(relatives[held], core, side), my_piece)
            climbed[side, held] = [send(a_all.at[where], a_all.at[where], (dp, m)) for m in above[1:]]

    def pass_on(stage, relative):
        for side in range(2):
            order = orders[side]
            held = sum(((relative >> i) & 1) << order[i] for i in range(stage))
            peer = (relatives[1 << order[stage]] * 2 + core, mp)
            where = (rows_of(relatives[held], core, side), my_piece)
            if held:
                arrive(side, held)
            spread[side, held | (1 << order[stage])] = send(a_all.at[where], a_all.at[where], peer)
            if held:
                climb(side, held)

    load_inverse.wait()
    for stage in range(stages):
        pass_on(stage, 0)
    crossed = [send(a_inverse, a_all.at[rows_of(chip, core)], partner)]

    def start_side(part, came, stage, side):
        first, last = chips >> (stage + 1), chips >> stage
        peer = (relatives[1 << orders[side][stage]] * 2 + core, mp)
        return send(part.at[side, first:last], came[stage].at[side], peer)

    def start(part, came, stage):
        return [start_side(part, came, stage, side) for side in range(2)]

    def add(part, came, stage, copies):
        for side in range(2):
            copies[side].wait_recv()
            count = chips >> (stage + 1)

            def one(slot, unused):
                total = part[side, slot].astype(full) + came[stage][side, slot].astype(full)
                part[side, slot] = total.astype(low)
                return unused

            lax.fori_loop(0, count, one, 0)

    def advance(part, came, copies):
        for stage in range(stages - 1):
            add(part, came, stage, copies)
            copies = start(part, came, stage + 1)
        return copies

    def choose(source, block_index, row, owner):
        rows = None
        for s in range(dp_count):
            cols = source[:, pl.ds(pl.multiple_of(block_index * block + s * strip, strip), strip)]
            rows = cols if rows is None else lax.select(owner_map[row, s] == owner, cols, rows)
        return rows

    def flip_strips(source, block_index, row):
        for r in range(chips):
            owner = relatives[r] * 2 + core
            span = max(strip, 128)
            rows = None
            for start_at in range(0, block, span):
                cols = source[:, pl.ds(pl.multiple_of(block_index * block + start_at, span), span)]
                held = owner_map[row, start_at // strip]
                for inner in range(1, span // strip):
                    held = jnp.where(owner_map[row, start_at // strip + inner] == owner, owner, held)
                rows = cols if rows is None else lax.select(held == owner, cols, rows)
            rows = rows.T
            for inner in range(span // strip):
                part = rows[inner * strip : (inner + 1) * strip]
                if inner == 0:
                    chosen = part
                    continue
                here = jnp.int32(0)
                for s in range(inner, dp_count, span // strip):
                    here = here + jnp.where(owner_map[row, s] == owner, jnp.int32(1), jnp.int32(0))
                chosen = lax.select(here == 1, part, chosen)
            flipped[0, r * strip : (r + 1) * strip, :] = chosen

    def turn(first):
        def one(j, unused):
            rows = pl.ds(pl.multiple_of(j * block, block), block)
            cols = pl.ds(pl.multiple_of(j * half, half), half)
            turned[first : first + own, cols] = jnp.dot(
                grads2[first : first + own, rows], g_cols[rows, :], preferred_element_type=full
            ).astype(low)
            return unused

        lax.fori_loop(0, ng, one, 0)

    with jax.named_scope("turn_own"):
        load_grads.wait()
        for copy in load_cols:
            copy.wait()
        turn(0)
    with jax.named_scope("pass_on"):
        for stage in range(1, stages):
            for relative in range(1, 1 << stage):
                pass_on(stage, relative)
    with jax.named_scope("turn_other"):
        other_grads.wait_recv()
        turn(own)

    def multiply(k):
        part = grad_part.at[k]
        came = [came.at[k] for came in grad_came]
        copies = []
        for first, last in ((chips // 2, chips), (0, chips // 2)):
            for side in range(2):
                if first:
                    if k < 2:
                        other_acts[2 * k + side].wait_recv()

                    def flip_one(v, unused):
                        cols = pl.ds(pl.multiple_of(k * block + side * half + v * 128, 128), 128)
                        rows = pl.ds(pl.multiple_of(v * 128, 128), 128)
                        flipped[side, rows, :] = acts2[:, cols].T
                        return unused

                    lax.fori_loop(0, half // 128, flip_one, 0)

                def product(slot, unused):
                    q = chip_at(chip, slot, orders[side])
                    cols = pl.ds(pl.multiple_of(q * width, width), width)
                    part[side, slot] = jnp.dot(
                        flipped[side], turned[:, cols], preferred_element_type=full
                    ).astype(low)
                    return unused

                lax.fori_loop(first, last, product, 0)
                if first:
                    copies.append(start_side(part, came, 0, side))
        return copies

    def advance_grad(k, copies):
        return advance(grad_part.at[k], [came.at[k] for came in grad_came], copies)

    def a_block(k, unused):
        flip_strips(acts2, k, k)
        for side in range(2):
            cols = pl.ds(pl.multiple_of(k * block + side * half, half), half)
            wide[...] = jnp.dot(flipped[0], acts2[:, cols], preferred_element_type=full)
            for r in range(chips):
                rows = wide[pl.ds(pl.multiple_of(r * strip + mp * sub, sub), sub), :]
                a_part[side, slot_of(r, orders[side]), k] = (rows / tokens).astype(low)
        return unused

    with jax.named_scope("wait_acts"):
        load_acts.wait()
    grad_copies = [None] * na
    with jax.named_scope("multiply0"):
        grad_copies[0] = multiply(0)

    with jax.named_scope("climb"):
        for r in range(1, chips):
            for side in range(2):
                arrive(side, r)
                climb(side, r)

    def g_block(j, unused):
        flip_strips(grads2, j, na + j)
        for side in range(2):
            cols = pl.ds(pl.multiple_of(j * block + side * half, half), half)
            wide[...] = jnp.dot(flipped[0], grads2[:, cols], preferred_element_type=full)
            for r in range(chips):
                rows = wide[r * strip : (r + 1) * strip, :]
                g_part[side, slot_of(r, orders[side]), j] = rows.astype(low)
        return unused

    def start_g():
        if not folded:
            lax.fori_loop(0, ng, g_block, 0)
            return start(g_part, g_came, 0)
        pick, tile, tile_came, tile_last, fold = sym

        def pick_strip(i, unused):
            r, other = lax.div(i, jnp.int32(2)), lax.rem(i, jnp.int32(2))
            owner = chip_at(chip, r, bits[::-1]) * 2 + other
            rows = choose(grads2, core, na + core, owner)
            at = pl.ds(pl.multiple_of(i * strip, strip), strip)
            pick[:, at] = rows
            flipped[lax.div(i, jnp.int32(dp_count // 2)), pl.ds(
                pl.multiple_of(lax.rem(i, jnp.int32(dp_count // 2)) * strip, strip), strip
            ), :] = rows.T
            return unused

        lax.fori_loop(0, dp_count, pick_strip, 0)

        def product(r, s, first=0, count=2):
            at = ((r % 2) * 2 + first) * strip
            lhs = flipped[r // 2, at : at + count * strip, :]
            rhs = pick[:, s * 2 * strip : (s + 1) * 2 * strip]
            return jnp.dot(lhs, rhs, preferred_element_type=full).astype(low)

        copies = [None, None]
        for part in (1, 0):
            for r in range(chips):
                for kind, s in enumerate((r, r ^ 3)):
                    sides = [
                        side for side in range(2)
                        if (slot_of(r, orders[side]) >= chips // 2) == bool(part)
                    ]
                    if not sides:
                        continue
                    value = product(r, s, sides[0], len(sides))
                    for i, side in enumerate(sides):
                        place = (0, 1, 3, 4)[slot_of(r, orders[side])]
                        tile[side, place, kind * strip : (kind + 1) * strip, :] = value[
                            i * strip : (i + 1) * strip
                        ]
            for side in range(2):
                near, far = 1 << orders[side][0], 1 << orders[side][1]
                if part:
                    tile[side, 5] = product(near, 3)
                    peer = (relatives[near] * 2 + core, mp)
                    copies[side] = send(tile.at[side, 3:6], tile_came.at[side], peer)
                else:
                    tile[side, 2] = product(0, far)
        return copies

    def advance_g(copies):
        if not folded:
            return advance(g_part, g_came, copies)
        pick, tile, tile_came, tile_last, fold = sym
        last = []
        for side in range(2):
            copies[side].wait_recv()

            def one(i, unused):
                total = tile[side, i].astype(full) + tile_came[side, i].astype(full)
                tile[side, i] = total.astype(low)
                return unused

            lax.fori_loop(0, 3, one, 0)
            peer = (relatives[1 << orders[side][1]] * 2 + core, mp)
            last.append(send(tile.at[side, 1:3], tile_last.at[side], peer))
        return last

    def finish_g(copies):
        if not folded:
            for side in range(2):
                copies[side].wait_recv()
                total = g_part[side, 0].astype(full) + g_came[-1][side, 0].astype(full)
                g_rows[:ng, :, side * half : (side + 1) * half] = total.astype(low)
            return None
        pick, tile, tile_came, tile_last, fold = sym
        for side in range(2):
            copies[side].wait_recv()
            turned_tile = tile_last[side, 1].astype(full).T
            fold[side] = tile[side, 2].astype(full) + turned_tile
            total = tile[side, 0].astype(full) + tile_last[side, 0].astype(full)
            for kind in range(2):
                fold[2 + kind, side * strip : (side + 1) * strip, :] = total[
                    kind * strip : (kind + 1) * strip
                ]
        for mine, other in ((1, 1 - core), (0, core)):
            rows = pl.ds(pl.multiple_of(other * strip, strip), strip)
            for s in range(dp_count):
                found = None
                for r, place in enumerate((2, 1, 0, 3)):
                    for c in range(2):
                        value = fold[place, rows, c * strip : (c + 1) * strip]
                        here = owner_map[na + core, s] == relatives[r] * 2 + c
                        found = value if found is None else lax.select(here, value, found)
                g_rows[mine, :, s * strip : (s + 1) * strip] = found.astype(low)
            if mine:
                copy = send(g_rows.at[1], g_rows.at[2], partner)
        return copy

    for k in range(1, na):
        with jax.named_scope(f"multiply{k}"):
            grad_copies[k] = multiply(k)
        if k == 1:
            with jax.named_scope("a_block"):
                load_map.wait()
                for later in range(4, 2 * na):
                    other_acts[later].wait_recv()
                lax.fori_loop(0, na, a_block, 0)
                a_copies = start(a_part, a_came, 0)
            with jax.named_scope("advance0"):
                grad_copies[0] = advance_grad(0, grad_copies[0])
            with jax.named_scope("start_g"):
                g_copies = start_g()
            with jax.named_scope("advance_a"):
                a_copies = advance(a_part, a_came, a_copies)
        else:
            with jax.named_scope(f"advance{k - 1}"):
                grad_copies[k - 1] = advance_grad(k - 1, grad_copies[k - 1])

    with jax.named_scope("advance_g"):
        g_copies = advance_g(g_copies)
    with jax.named_scope("gather_a"):
        for side in range(2):
            a_copies[side].wait_recv()
        for side in range(2):
            total = a_part[side, 0].astype(full) + a_came[-1][side, 0].astype(full)
            a_rows[mp, :, :, side * half : (side + 1) * half] = total.astype(low)
        gathered = [send(a_rows.at[mp], a_rows.at[mp], (dp, m)) for m in above[1:]]

    with jax.named_scope("cross"):
        for r in range(1, chips):
            for side in range(2):
                for copy in climbed[side, r]:
                    copy.wait_recv()
            where = a_all.at[rows_of(relatives[r], core)]
            crossed.append(send(where, where, partner))
    with jax.named_scope(f"advance{na - 1}"):
        grad_copies[na - 1] = advance_grad(na - 1, grad_copies[na - 1])
    with jax.named_scope("wait_cross"):
        for copy in crossed:
            copy.wait_recv()

    def finish(k):
        for side in range(2):
            grad_copies[k][side].wait_recv()
            total = grad_part[k, side, 0].astype(full) + grad_came[-1][k, side, 0].astype(full)
            right[side * half : (side + 1) * half, :] = total.astype(low)

        def rows_done(t, unused):
            rows = pl.ds(pl.multiple_of(k * block + t * 256, 256), 256)
            out_tile[rows, :] = jnp.dot(
                a_all[rows, :], right[...], preferred_element_type=full
            ).astype(low)
            return unused

        lax.fori_loop(0, block // 256, rows_done, 0)

    for k in range(na - 1):
        with jax.named_scope(f"finish{k}"):
            finish(k)
    with jax.named_scope("finish_g"):
        swapped = finish_g(g_copies)
        load_old_g.wait()

        def renew(j, rows):
            g_new[j] = decay_rate * g_old[j] + (1.0 - decay_rate) * rows.astype(full)

        if folded:
            renew(core, g_rows[0])
            swapped.wait_recv()
            renew(1 - core, g_rows[2])
        else:
            for j in range(ng):
                renew(j, g_rows[j])
    with jax.named_scope("wait_gather"):
        for copy in gathered:
            copy.wait_recv()
    with jax.named_scope("finish_a"):
        load_old_a.wait()
        for m in range(mp_count):
            rows = slice(m * sub, (m + 1) * sub)
            a_new[:, rows, :] = decay_rate * a_old[:, rows, :] + (1.0 - decay_rate) * a_rows[m].astype(full)
    with jax.named_scope(f"finish{na - 1}"):
        finish(na - 1)
    for copy in sent:
        copy.wait_send()


def store(*refs):
    count = len(refs) // 2
    copies = [
        pltpu.make_async_copy(refs[i], refs[count + i], refs[-1].at[i]) for i in range(count)
    ]
    for copy in copies:
        copy.start()
    for copy in copies:
        copy.wait()


def per_device(acts, grads_out, old_a, old_g, a_inverse, g_inverse, owner_map):
    dp_count = lax.axis_size("dp")
    mp_count = lax.axis_size("mp")
    chips = dp_count // 2
    stages = chips.bit_length() - 1
    own, features = acts.shape
    hidden = grads_out.shape[1]
    block = a_inverse.shape[1]
    na, ng = features // block, hidden // block
    strip = block // dp_count
    sub = strip // mp_count
    width = hidden // dp_count
    half = block // 2
    copies = 3 + 2 * na + (chips - 1) * (2 * mp_count + 1) + (na + 2) * 2 * stages + mp_count - 1
    loads = 6 + block // width // 2

    def came(*shape):
        return [pltpu.VMEM((*shape[0], chips >> (s + 1), *shape[1]), low) for s in range(stages)]

    scratch = [
        pltpu.VMEM((2 * own, features), low),
        pltpu.VMEM((2 * own, hidden), low),
        pltpu.VMEM((hidden, half), low),
        pltpu.VMEM((2 * own, hidden // 2), low),
        pltpu.VMEM((features, block), low),
        pltpu.VMEM((2, half, 2 * own), low),
        pltpu.VMEM((half, half), full),
        pltpu.VMEM((block, width), low),
        pltpu.VMEM((mp_count, na, sub, block), low),
        pltpu.VMEM((max(ng, 3), strip, block), low),
        pltpu.VMEM((na, strip, block), full),
        pltpu.VMEM((ng, strip, block), full),
        pltpu.SMEM((na + ng, dp_count), jnp.int32),
        pltpu.VMEM((na, 2, chips, half, width), low),
        pltpu.VMEM((2, chips, ng, strip, half), low),
        pltpu.VMEM((2, chips, na, sub, half), low),
        came((na, 2), (half, width)),
        came((2,), (ng, strip, half)),
        came((2,), (na, sub, half)),
        [
            pltpu.VMEM((2 * own, block), low),
            pltpu.VMEM((2, 6, 2 * strip, 2 * strip), low),
            pltpu.VMEM((2, 3, 2 * strip, 2 * strip), low),
            pltpu.VMEM((2, 2, 2 * strip, 2 * strip), low),
            pltpu.VMEM((4, 2 * strip, 2 * strip), full),
        ],
        pltpu.SemaphoreType.DMA((loads,)),
        pltpu.SemaphoreType.DMA((copies,)),
        pltpu.SemaphoreType.DMA((copies,)),
    ]
    outside = pl.BlockSpec(memory_space=pltpu.HBM)
    out, a_new, g_new = pl.pallas_call(
        functools.partial(kernel, (dp_count, mp_count, own * dp_count)),
        out_shape=(
            pltpu.VMEM((features, width), low),
            pltpu.VMEM((na, strip, block), full),
            pltpu.VMEM((ng, strip, block), full),
        ),
        in_specs=[outside] * 7,
        out_specs=(pl.BlockSpec(memory_space=pltpu.VMEM),) * 3,
        scratch_shapes=scratch,
        compiler_params=pltpu.CompilerParams(
            collective_id=0, has_side_effects=True, vmem_limit_bytes=59 * 1024 * 1024 + 7 * 1024 * 100
        ),
        name="step",
    )(owner_map, acts, grads_out, a_inverse, g_inverse, old_a, old_g)
    a_new, g_new, out = pl.pallas_call(
        store,
        out_shape=tuple(jax.ShapeDtypeStruct(x.shape, x.dtype) for x in (a_new, g_new, out)),
        in_specs=[pl.BlockSpec(memory_space=pltpu.VMEM)] * 3,
        out_specs=(pl.BlockSpec(memory_space=pl.ANY),) * 3,
        scratch_shapes=[pltpu.SemaphoreType.DMA((3,))],
        compiler_params=pltpu.CompilerParams(vmem_limit_bytes=1024 * 1024),
        name="store",
    )(a_new, g_new, out)
    return (a_new.reshape(old_a.shape), g_new.reshape(old_g.shape), out.reshape(features, 1, width))


def solution(mesh):
    placed = (
        P("dp", None),
        P("dp", "mp"),
        P("dp", None, None, None),
        P("mp", "dp", None, None, None),
        P("dp", None),
        P("mp", None),
        P(),
    )
    return jax.shard_map(
        per_device,
        mesh=mesh,
        in_specs=placed,
        out_specs=(P("dp", None, None, None), P("mp", "dp", None, None, None), P(None, "mp", "dp")),
        check_vma=False,
    )
```

```python
import functools

import jax
import jax.numpy as jnp
from jax import lax
from jax.experimental import pallas as pl
from jax.experimental.pallas import tpu as pltpu
from jax.sharding import PartitionSpec as P

decay_rate = 0.75
low = jnp.bfloat16
full = jnp.float32


def chip_at(me, slot, order):
    chip = 0
    for place, bit in enumerate(order):
        want = lax.rem(lax.div(jnp.int32(slot), jnp.int32(1 << (len(order) - 1 - place))), jnp.int32(2))
        have = lax.rem(lax.div(me, jnp.int32(1 << bit)), jnp.int32(2))
        chip = chip + (want + have - 2 * want * have) * (1 << bit)
    return chip


def slot_of(relative, order):
    slot = 0
    for place, bit in enumerate(order):
        slot += ((relative >> bit) & 1) << (len(order) - 1 - place)
    return slot


def kernel(
    sizes, map_in, acts, grads, a_inverse, g_inverse, old_a, old_g, out_tile, a_new, g_new,
    acts2, grads2, g_cols, turned, a_all, flipped, wide, right, sofar, a_rows, g_rows, a_old, g_old,
    owner_map, grad_part, g_part, a_part, grad_came, g_came, a_came, sym, local_sem, send_sem, recv_sem,
):
    dp_count, mp_count, tokens = sizes
    chips = dp_count // 2
    bits = list(range(chips.bit_length() - 1))
    orders = (bits, bits[::-1])
    stages = len(bits)
    own, features = acts.shape
    hidden = grads.shape[1]
    block = a_inverse.shape[1]
    na, ng = features // block, hidden // block
    strip = block // dp_count
    sub = strip // mp_count
    width = hidden // dp_count
    half = block // 2
    shard = a_inverse.shape[0]
    piece = block // mp_count

    dp = lax.axis_index("dp")
    mp = lax.axis_index("mp")
    chip, core = lax.div(dp, jnp.int32(2)), lax.rem(dp, jnp.int32(2))
    partner = (chip * 2 + 1 - core, mp)
    relatives = [chip_at(chip, r, bits[::-1]) for r in range(chips)]
    nook = strip + strip // 2
    one_slot = nook + 2 * strip
    starts = (0, one_slot, 2 * one_slot + 4 * strip, 3 * one_slot + 4 * strip, 2 * one_slot)
    starts += (4 * one_slot + 4 * strip,)
    folded = chips == 4 and ng == 2 and strip % 128 == 0
    above = [lax.rem(mp + step, jnp.int32(mp_count)) for step in range(mp_count)]

    sent = []

    def send(src, dst, device):
        place = len(sent)
        copy = pltpu.make_async_remote_copy(
            src_ref=src, dst_ref=dst, send_sem=send_sem.at[place], recv_sem=recv_sem.at[place],
            device_id=device, device_id_type=pl.DeviceIdType.MESH,
        )
        copy.start()
        sent.append(copy)
        return copy

    placed = []

    def move(src, dst):
        copy = pltpu.make_async_copy(src, dst, local_sem.at[len(placed)])
        copy.start()
        placed.append(copy)
        return copy

    def rows_of(chip_index, core_index, part=None):
        first = (chip_index * 2 + core_index) * shard
        if part is None:
            return pl.ds(pl.multiple_of(first, shard), shard)
        return pl.ds(pl.multiple_of(first + part * (shard // 2), shard // 2), shard // 2)

    my_piece = pl.ds(pl.multiple_of(mp * piece, piece), piece)

    load_inverse = move(a_inverse, a_all.at[rows_of(chip, core)])
    load_grads = move(grads, grads2.at[:own])
    load_cols = [
        move(
            g_inverse.at[:, pl.ds(pl.multiple_of((2 * u + core) * width, width), width)],
            g_cols.at[:, u * width : (u + 1) * width],
        )
        for u in range(block // width // 2)
    ]
    load_acts = move(acts, acts2.at[:own])
    load_map = move(map_in, owner_map)
    load_old_a = move(old_a.at[0], a_old)
    load_old_g = move(old_g.at[0, 0], g_old)

    with jax.named_scope("barrier"):
        barrier = pltpu.get_barrier_semaphore()
        peers = [partner]
        peers += [(q * 2 + core, mp) for q in relatives[1:]]
        peers += [(dp, m) for m in above[1:]]
        for peer in peers:
            pl.semaphore_signal(barrier, inc=1, device_id=peer, device_id_type=pl.DeviceIdType.MESH)
        pl.semaphore_wait(barrier, len(peers))

    spread = {}
    climbed = {}

    def arrive(side, held):
        if (side, held) not in climbed:
            spread[side, held].wait_recv()

    def climb(side, held):
        if (side, held) not in climbed:
            where = (rows_of(relatives[held], core, side), my_piece)
            climbed[side, held] = [send(a_all.at[where], a_all.at[where], (dp, m)) for m in above[1:]]

    def pass_on(stage, relative):
        for side in range(2):
            order = orders[side]
            held = sum(((relative >> i) & 1) << order[i] for i in range(stage))
            peer = (relatives[1 << order[stage]] * 2 + core, mp)
            where = (rows_of(relatives[held], core, side), my_piece)
            if held:
                arrive(side, held)
            spread[side, held | (1 << order[stage])] = send(a_all.at[where], a_all.at[where], peer)
            if held:
                climb(side, held)

    load_inverse.wait()
    for stage in range(stages):
        pass_on(stage, 0)
    other_grads = send(grads, grads2.at[own:], partner)
    other_acts = []

    def swap_acts(last):
        for i in range(len(other_acts), last):
            cols = slice(i * half, (i + 1) * half)
            other_acts.append(send(acts.at[:, cols], acts2.at[own:, cols], partner))

    swap_acts(2)

    def start_side(part, came, stage, side, slot=None, rows=None):
        first, last = chips >> (stage + 1), chips >> stage
        peer = (relatives[1 << orders[side][stage]] * 2 + core, mp)
        src, dst = part.at[side, first:last], came[stage].at[side]
        if slot is not None:
            src, dst = part.at[side, slot], came[stage].at[side, slot - first]
        if rows is not None:
            src, dst = src.at[:, rows], dst.at[:, rows]
        return send(src, dst, peer)

    def start(part, came, stage):
        return [[start_side(part, came, stage, side)] for side in range(2)]

    def wait_all(copies):
        for copy in copies:
            copy.wait_recv()

    def add(part, came, stage, copies):
        for side in range(2):
            wait_all(copies[side])
            count = chips >> (stage + 1)

            def one(slot, unused):
                total = part[side, slot].astype(full) + came[stage][side, slot].astype(full)
                part[side, slot] = total.astype(low)
                return unused

            lax.fori_loop(0, count, one, 0)

    def advance(part, came, copies, split=1):
        for stage in range(stages - 1):
            add(part, came, stage, copies)
            if stage < stages - 2 or split == 1:
                copies = start(part, came, stage + 1)
                continue
            step = part.shape[2] // split
            copies = [[], []]
            for i in range(split):
                for side in range(2):
                    rows = slice(i * step, (i + 1) * step)
                    copies[side].append(start_side(part, came, stage + 1, side, rows=rows))
        return copies

    def choose(source, block_index, row, owner):
        rows = None
        for s in range(dp_count):
            cols = source[:, pl.ds(pl.multiple_of(block_index * block + s * strip, strip), strip)]
            rows = cols if rows is None else lax.select(owner_map[row, s] == owner, cols, rows)
        return rows

    def flip_strips(source, block_index, row):
        for r in range(chips):
            owner = relatives[r] * 2 + core
            span = max(strip, 128)
            rows = None
            for start_at in range(0, block, span):
                cols = source[:, pl.ds(pl.multiple_of(block_index * block + start_at, span), span)]
                held = owner_map[row, start_at // strip]
                for inner in range(1, span // strip):
                    held = jnp.where(owner_map[row, start_at // strip + inner] == owner, owner, held)
                rows = cols if rows is None else lax.select(held == owner, cols, rows)
            rows = rows.T
            for inner in range(span // strip):
                part = rows[inner * strip : (inner + 1) * strip]
                if inner == 0:
                    chosen = part
                    continue
                here = jnp.int32(0)
                for s in range(inner, dp_count, span // strip):
                    here = here + jnp.where(owner_map[row, s] == owner, jnp.int32(1), jnp.int32(0))
                chosen = lax.select(here == 1, part, chosen)
            flipped[0, r * strip : (r + 1) * strip, :] = chosen

    def turn(first):
        def one(j, unused):
            rows = pl.ds(pl.multiple_of(j * block, block), block)
            cols = pl.ds(pl.multiple_of(j * half, half), half)
            turned[first : first + own, cols] = jnp.dot(
                grads2[first : first + own, rows], g_cols[rows, :], preferred_element_type=full
            ).astype(low)
            return unused

        lax.fori_loop(0, ng, one, 0)

    with jax.named_scope("turn_own"):
        load_grads.wait()
        for copy in load_cols:
            copy.wait()
        turn(0)
    def flip(k, side, first, last):
        def one(v, unused):
            cols = pl.ds(pl.multiple_of(k * block + side * half + v * 128, 128), 128)
            rows = pl.ds(pl.multiple_of(v * 128, 128), 128)
            flipped[side, rows, first:last] = acts2[first:last, cols].T
            return unused

        lax.fori_loop(0, half // 128, one, 0)

    with jax.named_scope("flip_own"):
        load_acts.wait()
        for side in range(2):
            flip(0, side, 0, own)
    with jax.named_scope("turn_other"):
        other_grads.wait_recv()
        turn(own)
    with jax.named_scope("pass_on"):
        swap_acts(2 * na)
        for stage in range(1, stages):
            for relative in range(1, 1 << stage):
                pass_on(stage, relative)
        crossed = [send(a_inverse, a_all.at[rows_of(chip, core)], partner)]

    def multiply(k):
        part = grad_part.at[k]
        came = [came.at[k] for came in grad_came]

        def product(side, slot):
            q = chip_at(chip, slot, orders[side])
            cols = pl.ds(pl.multiple_of(q * width, width), width)
            part[side, slot] = jnp.dot(
                flipped[side], turned[:, cols], preferred_element_type=full
            ).astype(low)

        def products(side, first, last):
            def one(slot, unused):
                product(side, slot)
                return unused

            lax.fori_loop(first, last, one, 0)

        copies = [[], []]
        if k == 0:
            for slot in range(chips - 1, chips // 2 - 1, -1):
                for side in range(2):
                    if slot == chips - 1:
                        other_acts[side].wait_recv()
                        flip(k, side, own, 2 * own)
                    product(side, slot)
                    copies[side].append(start_side(part, came, 0, side, slot))
        else:
            for side in range(2):
                if k == 1:
                    other_acts[2 * k + side].wait_recv()
                flip(k, side, 0, 2 * own)
                products(side, chips // 2, chips)
                copies[side].append(start_side(part, came, 0, side))
        for side in range(2):
            products(side, 0, chips // 2)
        return copies

    def advance_grad(k, copies):
        split = 2 if k == na - 1 and stages > 1 else 1
        return advance(grad_part.at[k], [came.at[k] for came in grad_came], copies, split)

    def a_block(k, unused):
        flip_strips(acts2, k, k)
        for side in range(2):
            cols = pl.ds(pl.multiple_of(k * block + side * half, half), half)
            wide[...] = jnp.dot(flipped[0], acts2[:, cols], preferred_element_type=full)
            for r in range(chips):
                rows = wide[pl.ds(pl.multiple_of(r * strip + mp * sub, sub), sub), :]
                a_part[side, slot_of(r, orders[side]), k] = (rows / tokens).astype(low)
        return unused

    grad_copies = [None] * na
    with jax.named_scope("multiply0"):
        grad_copies[0] = multiply(0)

    with jax.named_scope("climb"):
        for r in range(1, chips):
            for side in range(2):
                arrive(side, r)
                climb(side, r)

    def g_block(j, unused):
        flip_strips(grads2, j, na + j)
        for side in range(2):
            cols = pl.ds(pl.multiple_of(j * block + side * half, half), half)
            wide[...] = jnp.dot(flipped[0], grads2[:, cols], preferred_element_type=full)
            for r in range(chips):
                rows = wide[r * strip : (r + 1) * strip, :]
                g_part[side, slot_of(r, orders[side]), j] = rows.astype(low)
        return unused

    def start_g():
        if not folded:
            lax.fori_loop(0, ng, g_block, 0)
            return start(g_part, g_came, 0)
        pick, tile, tile_came, tile_last, fold = sym

        def pick_strip(i, unused):
            r, other = lax.div(i, jnp.int32(2)), lax.rem(i, jnp.int32(2))
            owner = chip_at(chip, r, bits[::-1]) * 2 + other
            rows = choose(grads2, core, na + core, owner)
            at = pl.ds(pl.multiple_of(i * strip, strip), strip)
            pick[:, at] = rows
            flipped[lax.div(i, jnp.int32(dp_count // 2)), pl.ds(
                pl.multiple_of(lax.rem(i, jnp.int32(dp_count // 2)) * strip, strip), strip
            ), :] = rows.T
            return unused

        lax.fori_loop(0, dp_count, pick_strip, 0)

        def product(r, first, count, s, col=0, cols=2):
            at = (r % 2) * 2 * strip + first
            lhs = flipped[r // 2, at : at + count, :]
            rhs = pick[:, (s * 2 + col) * strip : (s * 2 + col + cols) * strip]
            return jnp.dot(lhs, rhs, preferred_element_type=full).astype(low)

        def slot_tiles(r, side):
            at = starts[slot_of(r, orders[side])]
            if side == 0:
                value = product(r, 0, strip, r)
                tile[side, at : at + strip] = value[:, :strip]
                tile[side, at + strip : at + nook] = value[: strip // 2, strip:]
            else:
                tile[side, at : at + nook] = product(r, strip // 2, nook, r, 1, 1)
            value = product(r, side * strip, strip, r ^ 3)
            for c in range(2):
                first = at + nook + c * strip
                tile[side, first : first + strip] = value[:, c * strip : (c + 1) * strip]

        def pair_tile(r, s, side, at):
            value = product(r, 0, 2 * strip, s)
            for c in range(2):
                first = at + c * 2 * strip
                tile[side, first : first + 2 * strip] = value[:, c * strip : (c + 1) * strip]

        copies = []
        for upper in (True, False):
            for side in range(2):
                near, far = 1 << orders[side][0], 1 << orders[side][1]
                for r in range(chips):
                    if (slot_of(r, orders[side]) >= chips // 2) == upper:
                        slot_tiles(r, side)
                if upper:
                    pair_tile(near, 3, side, starts[5])
                    peer = (relatives[near] * 2 + core, mp)
                    copies.append(send(tile.at[side, starts[2] :], tile_came.at[side], peer))
                else:
                    pair_tile(0, far, side, starts[4])
        return copies

    def advance_g(copies):
        if not folded:
            return advance(g_part, g_came, copies)
        pick, tile, tile_came, tile_last, fold = sym
        last = []
        for side in range(2):
            copies[side].wait_recv()

            def one(i, unused):
                rows = pl.ds(pl.multiple_of(i * strip, strip), strip)
                total = tile[side, rows].astype(full) + tile_came[side, rows].astype(full)
                tile[side, rows] = total.astype(low)
                return unused

            lax.fori_loop(0, starts[2] // strip, one, 0)
            peer = (relatives[1 << orders[side][1]] * 2 + core, mp)
            last.append(send(tile.at[side, starts[1] : starts[2]], tile_last.at[side], peer))
        return last

    def finish_g(copies):
        if not folded:
            for side in range(2):
                wait_all(copies[side])
                total = g_part[side, 0].astype(full) + g_came[-1][side, 0].astype(full)
                g_rows[:ng, :, side * half : (side + 1) * half] = total.astype(low)
            return None
        pick, tile, tile_came, tile_last, fold = sym
        own_tiles = []
        for side in range(2):
            copies[side].wait_recv()

            def whole_tile(ref, at):
                parts = [ref[side, at + c * 2 * strip : at + (c + 1) * 2 * strip] for c in range(2)]
                return jnp.concatenate([part.astype(full) for part in parts], axis=1)

            fold[side] = whole_tile(tile, starts[4]) + whole_tile(tile_last, starts[1]).T
            total = tile[side, : starts[1]].astype(full) + tile_last[side, : starts[1]].astype(full)
            own_tiles.append(total[:nook])
            for c in range(2):
                first = nook + c * strip
                fold[3, side * strip : (side + 1) * strip, c * strip : (c + 1) * strip] = total[
                    first : first + strip
                ]
        cross = jnp.concatenate([own_tiles[0][strip:], own_tiles[1][: strip // 2]], axis=0)
        fold[2, :strip, :strip] = own_tiles[0][:strip]
        fold[2, :strip, strip:] = cross
        fold[2, strip:, :strip] = cross.T
        fold[2, strip:, strip:] = own_tiles[1][strip // 2 :]
        for mine, other in ((1, 1 - core), (0, core)):
            rows = pl.ds(pl.multiple_of(other * strip, strip), strip)
            for s in range(dp_count):
                found = None
                for r, place in enumerate((2, 1, 0, 3)):
                    for c in range(2):
                        value = fold[place, rows, c * strip : (c + 1) * strip]
                        here = owner_map[na + core, s] == relatives[r] * 2 + c
                        found = value if found is None else lax.select(here, value, found)
                g_rows[mine, :, s * strip : (s + 1) * strip] = found.astype(low)
            if mine:
                copy = send(g_rows.at[1], g_rows.at[2], partner)
        return copy

    for k in range(1, na):
        with jax.named_scope(f"multiply{k}"):
            grad_copies[k] = multiply(k)
        if k == 1:
            with jax.named_scope("a_block"):
                load_map.wait()
                for later in range(4, 2 * na):
                    other_acts[later].wait_recv()
                lax.fori_loop(0, na, a_block, 0)
                a_copies = start(a_part, a_came, 0)
            with jax.named_scope("advance0"):
                grad_copies[0] = advance_grad(0, grad_copies[0])
            with jax.named_scope("start_g"):
                g_copies = start_g()
            with jax.named_scope("advance_a"):
                a_copies = advance(a_part, a_came, a_copies)
        else:
            with jax.named_scope(f"advance{k - 1}"):
                grad_copies[k - 1] = advance_grad(k - 1, grad_copies[k - 1])

    with jax.named_scope("advance_g"):
        g_copies = advance_g(g_copies)
    with jax.named_scope("gather_a"):
        for side in range(2):
            wait_all(a_copies[side])
        for side in range(2):
            total = a_part[side, 0].astype(full) + a_came[-1][side, 0].astype(full)
            a_rows[mp, :, :, side * half : (side + 1) * half] = total.astype(low)
        gathered = [send(a_rows.at[mp], a_rows.at[mp], (dp, m)) for m in above[1:]]

    with jax.named_scope("cross"):
        for r in range(1, chips):
            for side in range(2):
                for copy in climbed[side, r]:
                    copy.wait_recv()
            where = a_all.at[rows_of(relatives[r], core)]
            crossed.append(send(where, where, partner))
    with jax.named_scope(f"advance{na - 1}"):
        grad_copies[na - 1] = advance_grad(na - 1, grad_copies[na - 1])
    with jax.named_scope("wait_cross"):
        for copy in crossed:
            copy.wait_recv()

    def finish(k):
        count = len(grad_copies[k][0]) if k == na - 1 else 1
        step = half // count
        for i in range(count):
            with jax.named_scope(f"finish{k}_{i}"):
                spans = []
                for side in range(2):
                    wait_all(grad_copies[k][side][i : i + 1])
                    rows = slice(i * step, (i + 1) * step)
                    total = (
                        grad_part[k, side, 0, rows].astype(full)
                        + grad_came[-1][k, side, 0, rows].astype(full)
                    )
                    spans.append(slice(side * half + i * step, side * half + (i + 1) * step))
                    right[spans[-1], :] = total.astype(low)
                if count == 1:
                    spans = [slice(0, block)]

                def rows_done(t, unused):
                    rows = pl.ds(pl.multiple_of(k * block + t * 256, 256), 256)
                    inner = pl.ds(pl.multiple_of(t * 256, 256), 256)
                    total = sum(
                        jnp.dot(a_all[rows, span], right[span, :], preferred_element_type=full)
                        for span in spans
                    )
                    if i:
                        total = total + sofar[inner, :]
                    if i < count - 1:
                        sofar[inner, :] = total
                    else:
                        out_tile[rows, :] = total.astype(low)
                    return unused

                lax.fori_loop(0, block // 256, rows_done, 0)

    for k in range(na - 1):
        finish(k)
    with jax.named_scope("finish_g"):
        swapped = finish_g(g_copies)
        load_old_g.wait()

        def renew(j, rows):
            g_new[j] = decay_rate * g_old[j] + (1.0 - decay_rate) * rows.astype(full)

        if folded:
            renew(core, g_rows[0])
            swapped.wait_recv()
            renew(1 - core, g_rows[2])
        else:
            for j in range(ng):
                renew(j, g_rows[j])
    with jax.named_scope("wait_gather"):
        for copy in gathered:
            copy.wait_recv()
    with jax.named_scope("finish_a"):
        load_old_a.wait()
        for m in range(mp_count):
            rows = slice(m * sub, (m + 1) * sub)
            a_new[:, rows, :] = decay_rate * a_old[:, rows, :] + (1.0 - decay_rate) * a_rows[m].astype(full)
    finish(na - 1)
    with jax.named_scope("drain"):
        for copy in sent:
            copy.wait_send()


def store(*refs):
    count = len(refs) // 2
    copies = [
        pltpu.make_async_copy(refs[i], refs[count + i], refs[-1].at[i]) for i in range(count)
    ]
    for copy in copies:
        copy.start()
    for copy in copies:
        copy.wait()


def per_device(acts, grads_out, old_a, old_g, a_inverse, g_inverse, owner_map):
    dp_count = lax.axis_size("dp")
    mp_count = lax.axis_size("mp")
    chips = dp_count // 2
    stages = chips.bit_length() - 1
    own, features = acts.shape
    hidden = grads_out.shape[1]
    block = a_inverse.shape[1]
    na, ng = features // block, hidden // block
    strip = block // dp_count
    sub = strip // mp_count
    width = hidden // dp_count
    half = block // 2
    copies = 5 + chips + 2 * na + (chips - 1) * (2 * mp_count + 1) + (na + 2) * 2 * stages + mp_count - 1
    loads = 6 + block // width // 2

    def came(*shape):
        return [pltpu.VMEM((*shape[0], chips >> (s + 1), *shape[1]), low) for s in range(stages)]

    scratch = [
        pltpu.VMEM((2 * own, features), low),
        pltpu.VMEM((2 * own, hidden), low),
        pltpu.VMEM((hidden, half), low),
        pltpu.VMEM((2 * own, hidden // 2), low),
        pltpu.VMEM((features, block), low),
        pltpu.VMEM((2, half, 2 * own), low),
        pltpu.VMEM((half, half), full),
        pltpu.VMEM((block, width), low),
        pltpu.VMEM((block, width), full),
        pltpu.VMEM((mp_count, na, sub, block), low),
        pltpu.VMEM((max(ng, 3), strip, block), low),
        pltpu.VMEM((na, strip, block), full),
        pltpu.VMEM((ng, strip, block), full),
        pltpu.SMEM((na + ng, dp_count), jnp.int32),
        pltpu.VMEM((na, 2, chips, half, width), low),
        pltpu.VMEM((2, chips, ng, strip, half), low),
        pltpu.VMEM((2, chips, na, sub, half), low),
        came((na, 2), (half, width)),
        came((2,), (ng, strip, half)),
        came((2,), (na, sub, half)),
        [
            pltpu.VMEM((2 * own, block), low),
            pltpu.VMEM((2, 22 * strip, strip), low),
            pltpu.VMEM((2, 11 * strip, strip), low),
            pltpu.VMEM((2, 15 * strip // 2, strip), low),
            pltpu.VMEM((4, 2 * strip, 2 * strip), full),
        ],
        pltpu.SemaphoreType.DMA((loads,)),
        pltpu.SemaphoreType.DMA((copies,)),
        pltpu.SemaphoreType.DMA((copies,)),
    ]
    outside = pl.BlockSpec(memory_space=pltpu.HBM)
    out, a_new, g_new = pl.pallas_call(
        functools.partial(kernel, (dp_count, mp_count, own * dp_count)),
        out_shape=(
            pltpu.VMEM((features, width), low),
            pltpu.VMEM((na, strip, block), full),
            pltpu.VMEM((ng, strip, block), full),
        ),
        in_specs=[outside] * 7,
        out_specs=(pl.BlockSpec(memory_space=pltpu.VMEM),) * 3,
        scratch_shapes=scratch,
        compiler_params=pltpu.CompilerParams(
            collective_id=0, has_side_effects=True, vmem_limit_bytes=59 * 1024 * 1024 + 7 * 1024 * 100
        ),
        name="step",
    )(owner_map, acts, grads_out, a_inverse, g_inverse, old_a, old_g)
    a_new, g_new, out = pl.pallas_call(
        store,
        out_shape=tuple(jax.ShapeDtypeStruct(x.shape, x.dtype) for x in (a_new, g_new, out)),
        in_specs=[pl.BlockSpec(memory_space=pltpu.VMEM)] * 3,
        out_specs=(pl.BlockSpec(memory_space=pl.ANY),) * 3,
        scratch_shapes=[pltpu.SemaphoreType.DMA((3,))],
        compiler_params=pltpu.CompilerParams(vmem_limit_bytes=1024 * 1024),
        name="store",
    )(a_new, g_new, out)
    return (a_new.reshape(old_a.shape), g_new.reshape(old_g.shape), out.reshape(features, 1, width))


def solution(mesh):
    placed = (
        P("dp", None),
        P("dp", "mp"),
        P("dp", None, None, None),
        P("mp", "dp", None, None, None),
        P("dp", None),
        P("mp", None),
        P(),
    )
    return jax.shard_map(
        per_device,
        mesh=mesh,
        in_specs=placed,
        out_specs=(P("dp", None, None, None), P("mp", "dp", None, None, None), P(None, "mp", "dp")),
        check_vma=False,
    )
```

```python
import functools

import jax
import jax.numpy as jnp
from jax import lax
from jax.experimental import pallas as pl
from jax.experimental.pallas import tpu as pltpu
from jax.sharding import PartitionSpec as P

decay_rate = 0.75
low = jnp.bfloat16
full = jnp.float32


def chip_at(me, slot, order):
    chip = 0
    for place, bit in enumerate(order):
        want = lax.rem(lax.div(jnp.int32(slot), jnp.int32(1 << (len(order) - 1 - place))), jnp.int32(2))
        have = lax.rem(lax.div(me, jnp.int32(1 << bit)), jnp.int32(2))
        chip = chip + (want + have - 2 * want * have) * (1 << bit)
    return chip


def slot_of(relative, order):
    slot = 0
    for place, bit in enumerate(order):
        slot += ((relative >> bit) & 1) << (len(order) - 1 - place)
    return slot


def kernel(
    sizes, map_in, acts, grads, a_inverse, g_inverse, old_a, old_g, out_tile, a_new, g_new, sofar, a_last, right,
    acts2, grads2, g_cols, turned, a_all, flipped, wide, a_rows, g_rows, a_old, g_old,
    owner_map, grad_part, g_part, a_part, grad_came, g_came, a_came, sym, local_sem, send_sem, recv_sem,
):
    dp_count, mp_count, tokens = sizes
    chips = dp_count // 2
    bits = list(range(chips.bit_length() - 1))
    orders = (bits, bits[::-1])
    stages = len(bits)
    own, features = acts.shape
    hidden = grads.shape[1]
    block = a_inverse.shape[1]
    na, ng = features // block, hidden // block
    strip = block // dp_count
    sub = strip // mp_count
    width = hidden // dp_count
    half = block // 2
    shard = a_inverse.shape[0]
    piece = block // mp_count

    dp = lax.axis_index("dp")
    mp = lax.axis_index("mp")
    chip, core = lax.div(dp, jnp.int32(2)), lax.rem(dp, jnp.int32(2))
    partner = (chip * 2 + 1 - core, mp)
    relatives = [chip_at(chip, r, bits[::-1]) for r in range(chips)]
    nook = strip + strip // 2
    one_slot = nook + 2 * strip
    starts = (0, one_slot, 2 * one_slot + 4 * strip, 3 * one_slot + 4 * strip, 2 * one_slot)
    starts += (4 * one_slot + 4 * strip,)
    folded = chips == 4 and ng == 2 and strip % 128 == 0
    above = [lax.rem(mp + step, jnp.int32(mp_count)) for step in range(mp_count)]

    out_names, in_names = {}, {}

    def send(src, dst, device, out_name, in_name):
        out_at = out_names.setdefault(out_name, len(out_names))
        in_at = in_names.setdefault(in_name, len(in_names))
        copy = pltpu.make_async_remote_copy(
            src_ref=src, dst_ref=dst, send_sem=send_sem.at[out_at], recv_sem=recv_sem.at[in_at],
            device_id=device, device_id_type=pl.DeviceIdType.MESH,
        )
        copy.start()

    def whole(ref, out_name, in_name):
        return pltpu.make_async_remote_copy(
            src_ref=ref, dst_ref=ref, send_sem=send_sem.at[out_names[out_name] if out_name else 0],
            recv_sem=recv_sem.at[in_names[in_name] if in_name else 0],
            device_id=partner, device_id_type=pl.DeviceIdType.MESH,
        )

    def arrived(name, ref):
        whole(ref, None, name).wait_recv()

    def left(name, ref):
        whole(ref, name, None).wait_send()

    placed = []

    def move(src, dst):
        copy = pltpu.make_async_copy(src, dst, local_sem.at[len(placed)])
        copy.start()
        placed.append(copy)
        return copy

    def rows_of(chip_index, core_index, part=None):
        first = (chip_index * 2 + core_index) * shard
        if part is None:
            return pl.ds(pl.multiple_of(first, shard), shard)
        return pl.ds(pl.multiple_of(first + part * (shard // 2), shard // 2), shard // 2)

    my_piece = pl.ds(pl.multiple_of(mp * piece, piece), piece)

    load_inverse = move(a_inverse, a_all.at[rows_of(chip, core)])
    load_grads = move(grads, grads2.at[:own])
    load_cols = [
        move(
            g_inverse.at[:, pl.ds(pl.multiple_of((2 * u + core) * width, width), width)],
            g_cols.at[:, u * width : (u + 1) * width],
        )
        for u in range(block // width // 2)
    ]
    load_acts = move(acts, acts2.at[:own])
    load_map = move(map_in, owner_map)
    load_old_a = move(old_a.at[0], a_old)
    load_old_g = move(old_g.at[0, 0], g_old)

    with jax.named_scope("barrier"):
        barrier = pltpu.get_barrier_semaphore()
        peers = [partner]
        peers += [(q * 2 + core, mp) for q in relatives[1:]]
        peers += [(dp, m) for m in above[1:]]
        for peer in peers:
            pl.semaphore_signal(barrier, inc=1, device_id=peer, device_id_type=pl.DeviceIdType.MESH)
        pl.semaphore_wait(barrier, len(peers))

    climbed = set()

    def piece_of(side, held):
        return a_all.at[rows_of(relatives[held], core, side), my_piece]

    def climb(side, held):
        if (side, held) not in climbed:
            climbed.add((side, held))
            arrived(("spread", side, held), piece_of(side, held))
            where = piece_of(side, held)
            for m in above[1:]:
                send(where, where, (dp, m), "climb", "climb")

    def pass_on(stage, relative):
        for side in range(2):
            order = orders[side]
            held = sum(((relative >> i) & 1) << order[i] for i in range(stage))
            peer = (relatives[1 << order[stage]] * 2 + core, mp)
            if held:
                climb(side, held)
            where = piece_of(side, held)
            name = ("spread", side, held | (1 << order[stage]))
            send(where, where, peer, "spread", name)

    load_inverse.wait()
    for stage in range(stages):
        pass_on(stage, 0)
    send(grads, grads2.at[own:], partner, "grads", "grads")

    def swap_acts(first, last):
        for i in range(first, last):
            cols = slice(i * half, (i + 1) * half)
            name = i if i < 2 else min(i // 2, 2)
            send(acts.at[:, cols], acts2.at[own:, cols], partner, "acts", ("acts", i < 2, name))

    swap_acts(0, 2)

    def start_side(name, part, came, stage, side, slot=None, rows=None):
        first, last = chips >> (stage + 1), chips >> stage
        peer = (relatives[1 << orders[side][stage]] * 2 + core, mp)
        src, dst = part.at[side, first:last], came[stage].at[side]
        if slot is not None:
            src, dst = part.at[side, slot], came[stage].at[side, slot - first]
        in_name = (name, stage, 0)
        if rows is not None:
            src, dst = src.at[:, rows], dst.at[:, rows]
            in_name = (name, stage, rows.start)
        send(src, dst, peer, name[0], in_name)

    def start(name, part, came, stage):
        for side in range(2):
            start_side(name, part, came, stage, side)

    def add(name, part, came, stage):
        arrived((name, stage, 0), came[stage])
        count = chips >> (stage + 1)
        for side in range(2):

            def one(slot, unused):
                total = part[side, slot].astype(full) + came[stage][side, slot].astype(full)
                part[side, slot] = total.astype(low)
                return unused

            lax.fori_loop(0, count, one, 0)

    def advance(name, part, came, split=1):
        for stage in range(stages - 1):
            add(name, part, came, stage)
            if stage < stages - 2 or split == 1:
                start(name, part, came, stage + 1)
                continue
            step = part.shape[2] // split
            for i in range(split):
                for side in range(2):
                    rows = slice(i * step, (i + 1) * step)
                    start_side(name, part, came, stage + 1, side, rows=rows)

    def choose(source, block_index, row, owner):
        rows = None
        for s in range(dp_count):
            cols = source[:, pl.ds(pl.multiple_of(block_index * block + s * strip, strip), strip)]
            rows = cols if rows is None else lax.select(owner_map[row, s] == owner, cols, rows)
        return rows

    def flip_strips(source, block_index, row):
        for r in range(chips):
            owner = relatives[r] * 2 + core
            span = max(strip, 128)
            rows = None
            for start_at in range(0, block, span):
                cols = source[:, pl.ds(pl.multiple_of(block_index * block + start_at, span), span)]
                held = owner_map[row, start_at // strip]
                for inner in range(1, span // strip):
                    held = jnp.where(owner_map[row, start_at // strip + inner] == owner, owner, held)
                rows = cols if rows is None else lax.select(held == owner, cols, rows)
            rows = rows.T
            for inner in range(span // strip):
                part = rows[inner * strip : (inner + 1) * strip]
                if inner == 0:
                    chosen = part
                    continue
                here = jnp.int32(0)
                for s in range(inner, dp_count, span // strip):
                    here = here + jnp.where(owner_map[row, s] == owner, jnp.int32(1), jnp.int32(0))
                chosen = lax.select(here == 1, part, chosen)
            flipped[0, r * strip : (r + 1) * strip, :] = chosen

    def turn(first):
        def one(j, unused):
            rows = pl.ds(pl.multiple_of(j * block, block), block)
            cols = pl.ds(pl.multiple_of(j * half, half), half)
            turned[first : first + own, cols] = jnp.dot(
                grads2[first : first + own, rows], g_cols[rows, :], preferred_element_type=full
            ).astype(low)
            return unused

        lax.fori_loop(0, ng, one, 0)

    with jax.named_scope("turn_own"):
        load_grads.wait()
        for copy in load_cols:
            copy.wait()
        turn(0)
    def flip(k, side, first, last):
        def one(v, unused):
            cols = pl.ds(pl.multiple_of(k * block + side * half + v * 128, 128), 128)
            rows = pl.ds(pl.multiple_of(v * 128, 128), 128)
            flipped[side, rows, first:last] = acts2[first:last, cols].T
            return unused

        lax.fori_loop(0, half // 128, one, 0)

    with jax.named_scope("flip_own"):
        load_acts.wait()
        for side in range(2):
            flip(0, side, 0, own)
    with jax.named_scope("turn_other"):
        arrived("grads", grads2.at[own:])
        turn(own)
    with jax.named_scope("pass_on"):
        swap_acts(2, 2 * na)
        for stage in range(1, stages):
            for relative in range(1, 1 << stage):
                pass_on(stage, relative)
        send(a_inverse, a_all.at[rows_of(chip, core)], partner, "cross", "cross")

    def multiply(k):
        part = grad_part.at[k]
        came = [came.at[k] for came in grad_came]

        def product(side, slot):
            q = chip_at(chip, slot, orders[side])
            cols = pl.ds(pl.multiple_of(q * width, width), width)
            part[side, slot] = jnp.dot(
                flipped[side], turned[:, cols], preferred_element_type=full
            ).astype(low)

        def products(side, first, last):
            def one(slot, unused):
                product(side, slot)
                return unused

            lax.fori_loop(first, last, one, 0)

        if k == 0:
            for slot in range(chips - 1, chips // 2 - 1, -1):
                for side in range(2):
                    if slot == chips - 1:
                        arrived(("acts", True, side), acts2.at[own:, side * half : (side + 1) * half])
                        flip(k, side, own, 2 * own)
                    product(side, slot)
                    start_side(("grad", k), part, came, 0, side, slot)
        else:
            for side in range(2):
                flip(k, side, 0, 2 * own)
                products(side, chips // 2, chips)
                start_side(("grad", k), part, came, 0, side)
        for side in range(2):
            products(side, 0, chips // 2)

    def advance_grad(k):
        split = 2 if k == na - 1 and stages > 1 else 1
        advance(("grad", k), grad_part.at[k], [came.at[k] for came in grad_came], split)

    def a_block(k, unused):
        flip_strips(acts2, k, k)
        for side in range(2):
            cols = pl.ds(pl.multiple_of(k * block + side * half, half), half)
            wide[...] = jnp.dot(flipped[0], acts2[:, cols], preferred_element_type=full)
            for r in range(chips):
                rows = wide[pl.ds(pl.multiple_of(r * strip + mp * sub, sub), sub), :]
                a_part[side, slot_of(r, orders[side]), k] = (rows / tokens).astype(low)
        return unused

    with jax.named_scope("multiply0"):
        multiply(0)

    with jax.named_scope("climb"):
        for r in range(1, chips):
            for side in range(2):
                climb(side, r)

    def g_block(j, unused):
        flip_strips(grads2, j, na + j)
        for side in range(2):
            cols = pl.ds(pl.multiple_of(j * block + side * half, half), half)
            wide[...] = jnp.dot(flipped[0], grads2[:, cols], preferred_element_type=full)
            for r in range(chips):
                rows = wide[r * strip : (r + 1) * strip, :]
                g_part[side, slot_of(r, orders[side]), j] = rows.astype(low)
        return unused

    def start_g():
        if not folded:
            lax.fori_loop(0, ng, g_block, 0)
            start(("g",), g_part, g_came, 0)
            return
        pick, tile, tile_came, tile_last, fold = sym

        def pick_strip(i, unused):
            r, other = lax.div(i, jnp.int32(2)), lax.rem(i, jnp.int32(2))
            owner = chip_at(chip, r, bits[::-1]) * 2 + other
            rows = choose(grads2, core, na + core, owner)
            at = pl.ds(pl.multiple_of(i * strip, strip), strip)
            pick[:, at] = rows
            flipped[lax.div(i, jnp.int32(dp_count // 2)), pl.ds(
                pl.multiple_of(lax.rem(i, jnp.int32(dp_count // 2)) * strip, strip), strip
            ), :] = rows.T
            return unused

        lax.fori_loop(0, dp_count, pick_strip, 0)

        def product(r, first, count, s, col=0, cols=2):
            at = (r % 2) * 2 * strip + first
            lhs = flipped[r // 2, at : at + count, :]
            rhs = pick[:, (s * 2 + col) * strip : (s * 2 + col + cols) * strip]
            return jnp.dot(lhs, rhs, preferred_element_type=full).astype(low)

        def slot_tiles(r, side):
            at = starts[slot_of(r, orders[side])]
            if side == 0:
                value = product(r, 0, strip, r)
                tile[side, at : at + strip] = value[:, :strip]
                tile[side, at + strip : at + nook] = value[: strip // 2, strip:]
            else:
                tile[side, at : at + nook] = product(r, strip // 2, nook, r, 1, 1)
            value = product(r, side * strip, strip, r ^ 3)
            for c in range(2):
                first = at + nook + c * strip
                tile[side, first : first + strip] = value[:, c * strip : (c + 1) * strip]

        def pair_tile(r, s, side, at):
            value = product(r, 0, 2 * strip, s)
            for c in range(2):
                first = at + c * 2 * strip
                tile[side, first : first + 2 * strip] = value[:, c * strip : (c + 1) * strip]

        for upper in (True, False):
            for side in range(2):
                near, far = 1 << orders[side][0], 1 << orders[side][1]
                for r in range(chips):
                    if (slot_of(r, orders[side]) >= chips // 2) == upper:
                        slot_tiles(r, side)
                if upper:
                    pair_tile(near, 3, side, starts[5])
                    peer = (relatives[near] * 2 + core, mp)
                    send(tile.at[side, starts[2] :], tile_came.at[side], peer, "g", "tile0")
                else:
                    pair_tile(0, far, side, starts[4])

    def advance_g():
        if not folded:
            advance(("g",), g_part, g_came)
            return
        pick, tile, tile_came, tile_last, fold = sym
        arrived("tile0", tile_came)
        for side in range(2):

            def one(i, unused):
                rows = pl.ds(pl.multiple_of(i * strip, strip), strip)
                total = tile[side, rows].astype(full) + tile_came[side, rows].astype(full)
                tile[side, rows] = total.astype(low)
                return unused

            lax.fori_loop(0, starts[2] // strip, one, 0)
            peer = (relatives[1 << orders[side][1]] * 2 + core, mp)
            send(tile.at[side, starts[1] : starts[2]], tile_last.at[side], peer, "g", "tile1")

    def finish_g():
        if not folded:
            arrived((("g",), stages - 1, 0), g_came[-1])
            for side in range(2):
                total = g_part[side, 0].astype(full) + g_came[-1][side, 0].astype(full)
                g_rows[:ng, :, side * half : (side + 1) * half] = total.astype(low)
            return
        pick, tile, tile_came, tile_last, fold = sym
        own_tiles = []
        arrived("tile1", tile_last)
        for side in range(2):

            def whole_tile(ref, at):
                parts = [ref[side, at + c * 2 * strip : at + (c + 1) * 2 * strip] for c in range(2)]
                return jnp.concatenate([part.astype(full) for part in parts], axis=1)

            fold[side] = whole_tile(tile, starts[4]) + whole_tile(tile_last, starts[1]).T
            total = tile[side, : starts[1]].astype(full) + tile_last[side, : starts[1]].astype(full)
            own_tiles.append(total[:nook])
            for c in range(2):
                first = nook + c * strip
                fold[3, side * strip : (side + 1) * strip, c * strip : (c + 1) * strip] = total[
                    first : first + strip
                ]
        cross = jnp.concatenate([own_tiles[0][strip:], own_tiles[1][: strip // 2]], axis=0)
        fold[2, :strip, :strip] = own_tiles[0][:strip]
        fold[2, :strip, strip:] = cross
        fold[2, strip:, :strip] = cross.T
        fold[2, strip:, strip:] = own_tiles[1][strip // 2 :]
        for mine, other in ((1, 1 - core), (0, core)):
            rows = pl.ds(pl.multiple_of(other * strip, strip), strip)
            for s in range(dp_count):
                found = None
                for r, place in enumerate((2, 1, 0, 3)):
                    for c in range(2):
                        value = fold[place, rows, c * strip : (c + 1) * strip]
                        here = owner_map[na + core, s] == relatives[r] * 2 + c
                        found = value if found is None else lax.select(here, value, found)
                g_rows[mine, :, s * strip : (s + 1) * strip] = found.astype(low)
            if mine:
                send(g_rows.at[1], g_rows.at[2], partner, "rows", "rows")

    for k in range(1, na):
        with jax.named_scope(f"multiply{k}"):
            if k == 1:
                arrived(("acts", False, 1), acts2.at[own:, block : 2 * block])
            multiply(k)
        if k == 1:
            with jax.named_scope("a_block"):
                load_map.wait()
                if na > 2:
                    arrived(("acts", False, 2), acts2.at[own:, 2 * block :])
                lax.fori_loop(0, na, a_block, 0)
                start(("a",), a_part, a_came, 0)
            with jax.named_scope("advance0"):
                advance_grad(0)
            with jax.named_scope("start_g"):
                start_g()
            with jax.named_scope("advance_a"):
                advance(("a",), a_part, a_came)
        else:
            with jax.named_scope(f"advance{k - 1}"):
                advance_grad(k - 1)

    with jax.named_scope("advance_g"):
        advance_g()
    with jax.named_scope("gather_a"):
        arrived((("a",), stages - 1, 0), a_came[-1])
        for side in range(2):
            total = a_part[side, 0].astype(full) + a_came[-1][side, 0].astype(full)
            a_rows[mp, :, :, side * half : (side + 1) * half] = total.astype(low)
        for m in above[1:]:
            send(a_rows.at[mp], a_rows.at[mp], (dp, m), "gather", "gather")

    climbing = a_all.at[: (chips - 1) * shard, : (mp_count - 1) * piece]
    with jax.named_scope("cross"):
        arrived("climb", climbing)
        for r in range(1, chips):
            where = a_all.at[rows_of(relatives[r], core)]
            send(where, where, partner, "cross", "cross")
    with jax.named_scope(f"advance{na - 1}"):
        advance_grad(na - 1)
    with jax.named_scope("wait_cross"):
        arrived("cross", a_all.at[: chips * shard])

    def finish(k, piece_index=0, count=1):
        step = half // count
        spans = []
        name = (("grad", k), stages - 1, piece_index * step)
        rows = slice(piece_index * step, (piece_index + 1) * step)
        arrived(name, grad_came[-1].at[k, :, :, rows])
        for side in range(2):
            total = (
                grad_part[k, side, 0, rows].astype(full) + grad_came[-1][k, side, 0, rows].astype(full)
            )
            spans.append(slice(side * half + rows.start, side * half + rows.stop))
            right[spans[-1], :] = total.astype(low)
        if piece_index:
            return
        if count == 1:
            spans = [slice(0, block)]

        def rows_done(t, unused):
            rows = pl.ds(pl.multiple_of(k * block + t * 256, 256), 256)
            inner = pl.ds(pl.multiple_of(t * 256, 256), 256)
            total = sum(
                jnp.dot(a_all[rows, span], right[span, :], preferred_element_type=full)
                for span in spans
            )
            if count > 1:
                sofar[inner, :] = total
                a_last[inner, :] = a_all[rows, :]
            else:
                out_tile[rows, :] = total.astype(low)
            return unused

        lax.fori_loop(0, block // 256, rows_done, 0)

    for k in range(na - 1):
        finish(k)
    with jax.named_scope("finish_g"):
        finish_g()
        load_old_g.wait()

        def renew(j, rows):
            g_new[j] = decay_rate * g_old[j] + (1.0 - decay_rate) * rows.astype(full)

        if folded:
            renew(core, g_rows[0])
            arrived("rows", g_rows.at[2])
            renew(1 - core, g_rows[2])
        else:
            for j in range(ng):
                renew(j, g_rows[j])
    with jax.named_scope("wait_gather"):
        arrived("gather", a_rows.at[: mp_count - 1])
    with jax.named_scope("finish_a"):
        load_old_a.wait()
        for m in range(mp_count):
            rows = slice(m * sub, (m + 1) * sub)
            a_new[:, rows, :] = decay_rate * a_old[:, rows, :] + (1.0 - decay_rate) * a_rows[m].astype(full)
    with jax.named_scope("finish_first"):
        finish(na - 1, 0, 2)
    with jax.named_scope("finish_last"):
        finish(na - 1, 1, 2)
    with jax.named_scope("drain"):
        left("grads", grads2.at[own:])
        left("acts", acts2.at[own:])
        left("spread", a_all.at[: (chips - 1) * shard, :piece])
        left("climb", climbing)
        left("cross", a_all.at[: chips * shard])
        left("grad", grad_part.at[:, :, : chips - 1])
        left("a", a_part.at[:, : chips - 1])
        if folded:
            left("g", sym[1].at[:, : 2 * starts[2] - starts[1]])
            left("rows", g_rows.at[1])
        else:
            left("g", g_part.at[:, : chips - 1])
        left("gather", a_rows.at[: mp_count - 1])


def store(first, a_new, g_new, sofar, a_last, right, out, a_out, g_out, last, sem):
    copies = [
        pltpu.make_async_copy(a_new, a_out, sem.at[0]),
        pltpu.make_async_copy(g_new, g_out, sem.at[1]),
        pltpu.make_async_copy(first, out.at[: first.shape[0]], sem.at[2]),
    ]
    for copy in copies:
        copy.start()
    block = a_last.shape[0]
    quarter = block // 4

    def one(t, unused):
        rows = pl.ds(pl.multiple_of(t * 256, 256), 256)
        total = sofar[rows, :]
        for begin in (quarter, 3 * quarter):
            span = slice(begin, begin + quarter)
            total += jnp.dot(a_last[rows, span], right[span, :], preferred_element_type=full)
        last[rows, :] = total.astype(low)
        return unused

    lax.fori_loop(0, block // 256, one, 0)
    copies.append(pltpu.make_async_copy(last, out.at[first.shape[0] :], sem.at[3]))
    copies[-1].start()
    for copy in copies:
        copy.wait()


def per_device(acts, grads_out, old_a, old_g, a_inverse, g_inverse, owner_map):
    dp_count = lax.axis_size("dp")
    mp_count = lax.axis_size("mp")
    chips = dp_count // 2
    stages = chips.bit_length() - 1
    own, features = acts.shape
    hidden = grads_out.shape[1]
    block = a_inverse.shape[1]
    na, ng = features // block, hidden // block
    strip = block // dp_count
    sub = strip // mp_count
    width = hidden // dp_count
    half = block // 2
    names_out = 10
    names_in = 9 + 2 * (chips - 1) + (na + 2) * stages + 1
    loads = 6 + block // width // 2

    def came(*shape):
        return [pltpu.VMEM((*shape[0], chips >> (s + 1), *shape[1]), low) for s in range(stages)]

    scratch = [
        pltpu.VMEM((2 * own, features), low),
        pltpu.VMEM((2 * own, hidden), low),
        pltpu.VMEM((hidden, half), low),
        pltpu.VMEM((2 * own, hidden // 2), low),
        pltpu.VMEM((features, block), low),
        pltpu.VMEM((2, half, 2 * own), low),
        pltpu.VMEM((half, half), full),
        pltpu.VMEM((mp_count, na, sub, block), low),
        pltpu.VMEM((max(ng, 3), strip, block), low),
        pltpu.VMEM((na, strip, block), full),
        pltpu.VMEM((ng, strip, block), full),
        pltpu.SMEM((na + ng, dp_count), jnp.int32),
        pltpu.VMEM((na, 2, chips, half, width), low),
        pltpu.VMEM((2, chips, ng, strip, half), low),
        pltpu.VMEM((2, chips, na, sub, half), low),
        came((na, 2), (half, width)),
        came((2,), (ng, strip, half)),
        came((2,), (na, sub, half)),
        [
            pltpu.VMEM((2 * own, block), low),
            pltpu.VMEM((2, 22 * strip, strip), low),
            pltpu.VMEM((2, 11 * strip, strip), low),
            pltpu.VMEM((2, 15 * strip // 2, strip), low),
            pltpu.VMEM((4, 2 * strip, 2 * strip), full),
        ],
        pltpu.SemaphoreType.DMA((loads,)),
        pltpu.SemaphoreType.DMA((names_out,)),
        pltpu.SemaphoreType.DMA((names_in,)),
    ]
    outside = pl.BlockSpec(memory_space=pltpu.HBM)
    results = pl.pallas_call(
        functools.partial(kernel, (dp_count, mp_count, own * dp_count)),
        out_shape=(
            pltpu.VMEM((features - block, width), low),
            pltpu.VMEM((na, strip, block), full),
            pltpu.VMEM((ng, strip, block), full),
            pltpu.VMEM((block, width), full),
            pltpu.VMEM((block, block), low),
            pltpu.VMEM((block, width), low),
        ),
        in_specs=[outside] * 7,
        out_specs=(pl.BlockSpec(memory_space=pltpu.VMEM),) * 6,
        scratch_shapes=scratch,
        compiler_params=pltpu.CompilerParams(
            collective_id=0, has_side_effects=True, vmem_limit_bytes=57 * 1024 * 1024 - 300 * 1024
        ),
        name="step",
    )(owner_map, acts, grads_out, a_inverse, g_inverse, old_a, old_g)
    out, a_new, g_new = pl.pallas_call(
        store,
        out_shape=(
            jax.ShapeDtypeStruct((features, width), low),
            jax.ShapeDtypeStruct((na, strip, block), full),
            jax.ShapeDtypeStruct((ng, strip, block), full),
        ),
        in_specs=[pl.BlockSpec(memory_space=pltpu.VMEM)] * 6,
        out_specs=(pl.BlockSpec(memory_space=pl.ANY),) * 3,
        scratch_shapes=[pltpu.VMEM((block, width), low), pltpu.SemaphoreType.DMA((4,))],
        compiler_params=pltpu.CompilerParams(vmem_limit_bytes=8 * 1024 * 1024),
        name="store",
    )(*results)
    return (a_new.reshape(old_a.shape), g_new.reshape(old_g.shape), out.reshape(features, 1, width))


def solution(mesh):
    placed = (
        P("dp", None),
        P("dp", "mp"),
        P("dp", None, None, None),
        P("mp", "dp", None, None, None),
        P("dp", None),
        P("mp", None),
        P(),
    )
    return jax.shard_map(
        per_device,
        mesh=mesh,
        in_specs=placed,
        out_specs=(P("dp", None, None, None), P("mp", "dp", None, None, None), P(None, "mp", "dp")),
        check_vma=False,
    )
```

```python
import functools

import jax
import jax.numpy as jnp
from jax import lax
from jax.experimental import pallas as pl
from jax.experimental.pallas import tpu as pltpu
from jax.sharding import PartitionSpec as P

decay_rate = 0.75
low = jnp.bfloat16
full = jnp.float32


def chip_at(me, slot, order):
    chip = 0
    for place, bit in enumerate(order):
        want = lax.rem(lax.div(jnp.int32(slot), jnp.int32(1 << (len(order) - 1 - place))), jnp.int32(2))
        have = lax.rem(lax.div(me, jnp.int32(1 << bit)), jnp.int32(2))
        chip = chip + (want + have - 2 * want * have) * (1 << bit)
    return chip


def slot_of(relative, order):
    slot = 0
    for place, bit in enumerate(order):
        slot += ((relative >> bit) & 1) << (len(order) - 1 - place)
    return slot


def kernel(
    sizes, map_in, acts, grads, a_inverse, g_inverse, old_a, old_g, out_tile, a_new, g_new, sofar, a_last, right,
    acts2, grads2, g_cols, turned, a_all, flipped, wide, a_rows, g_rows, a_old, g_old,
    owner_map, grad_part, g_part, a_part, grad_came, g_came, a_came, sym, local_sem, send_sem, recv_sem,
):
    dp_count, mp_count, tokens = sizes
    chips = dp_count // 2
    bits = list(range(chips.bit_length() - 1))
    orders = (bits, bits[::-1])
    stages = len(bits)
    own, features = acts.shape
    hidden = grads.shape[1]
    block = a_inverse.shape[1]
    na, ng = features // block, hidden // block
    strip = block // dp_count
    sub = strip // mp_count
    width = hidden // dp_count
    half = block // 2
    shard = a_inverse.shape[0]
    piece = block // mp_count

    dp = lax.axis_index("dp")
    mp = lax.axis_index("mp")
    chip, core = lax.div(dp, jnp.int32(2)), lax.rem(dp, jnp.int32(2))
    partner = (chip * 2 + 1 - core, mp)
    relatives = [chip_at(chip, r, bits[::-1]) for r in range(chips)]
    nook = strip + strip // 2
    one_slot = nook + 2 * strip
    starts = (0, one_slot, 2 * one_slot + 4 * strip, 3 * one_slot + 4 * strip, 2 * one_slot)
    starts += (4 * one_slot + 4 * strip,)
    folded = chips == 4 and ng == 2 and strip % 128 == 0
    above = [lax.rem(mp + step, jnp.int32(mp_count)) for step in range(mp_count)]

    out_names, in_names = {}, {}

    def send(src, dst, device, out_name, in_name):
        out_at = out_names.setdefault(out_name, len(out_names))
        in_at = in_names.setdefault(in_name, len(in_names))
        copy = pltpu.make_async_remote_copy(
            src_ref=src, dst_ref=dst, send_sem=send_sem.at[out_at], recv_sem=recv_sem.at[in_at],
            device_id=device, device_id_type=pl.DeviceIdType.MESH,
        )
        copy.start()

    def whole(ref, out_name, in_name):
        return pltpu.make_async_remote_copy(
            src_ref=ref, dst_ref=ref, send_sem=send_sem.at[out_names[out_name] if out_name else 0],
            recv_sem=recv_sem.at[in_names[in_name] if in_name else 0],
            device_id=partner, device_id_type=pl.DeviceIdType.MESH,
        )

    def arrived(name, ref):
        whole(ref, None, name).wait_recv()

    def left(name, ref):
        whole(ref, name, None).wait_send()

    placed = []

    def move(src, dst):
        copy = pltpu.make_async_copy(src, dst, local_sem.at[len(placed)])
        copy.start()
        placed.append(copy)
        return copy

    def rows_of(chip_index, core_index, part=None):
        first = (chip_index * 2 + core_index) * shard
        if part is None:
            return pl.ds(pl.multiple_of(first, shard), shard)
        return pl.ds(pl.multiple_of(first + part * (shard // 2), shard // 2), shard // 2)

    my_piece = pl.ds(pl.multiple_of(mp * piece, piece), piece)

    load_inverse = move(a_inverse, a_all.at[rows_of(chip, core)])
    load_grads = move(grads, grads2.at[:own])
    load_cols = [
        move(
            g_inverse.at[:, pl.ds(pl.multiple_of((2 * u + core) * width, width), width)],
            g_cols.at[:, u * width : (u + 1) * width],
        )
        for u in range(block // width // 2)
    ]
    load_acts = move(acts, acts2.at[:own])
    load_map = move(map_in, owner_map)
    load_old_a = move(old_a.at[0], a_old)
    load_old_g = move(old_g.at[0, 0], g_old)

    with jax.named_scope("barrier"):
        barrier = pltpu.get_barrier_semaphore()
        peers = [partner]
        peers += [(q * 2 + core, mp) for q in relatives[1:]]
        peers += [(dp, m) for m in above[1:]]
        for peer in peers:
            pl.semaphore_signal(barrier, inc=1, device_id=peer, device_id_type=pl.DeviceIdType.MESH)
        pl.semaphore_wait(barrier, len(peers))

    climbed = set()

    def piece_of(side, held):
        return a_all.at[rows_of(relatives[held], core, side), my_piece]

    def climb(side, held):
        if (side, held) not in climbed:
            climbed.add((side, held))
            arrived(("spread", side, held), piece_of(side, held))
            where = piece_of(side, held)
            for m in above[1:]:
                send(where, where, (dp, m), "climb", "climb")

    def pass_on(stage, relative):
        for side in range(2):
            order = orders[side]
            held = sum(((relative >> i) & 1) << order[i] for i in range(stage))
            peer = (relatives[1 << order[stage]] * 2 + core, mp)
            if held:
                climb(side, held)
            where = piece_of(side, held)
            name = ("spread", side, held | (1 << order[stage]))
            send(where, where, peer, "spread", name)

    load_inverse.wait()
    for stage in range(stages):
        pass_on(stage, 0)
    send(grads, grads2.at[own:], partner, "grads", "grads")

    def swap_acts(first, last):
        for i in range(first, last):
            cols = slice(i * half, (i + 1) * half)
            name = i if i < 2 else min(i // 2, 2)
            send(acts.at[:, cols], acts2.at[own:, cols], partner, "acts", ("acts", i < 2, name))

    swap_acts(0, 2)

    def start_side(name, part, came, stage, side, slot=None, rows=None):
        first, last = chips >> (stage + 1), chips >> stage
        peer = (relatives[1 << orders[side][stage]] * 2 + core, mp)
        src, dst = part.at[side, first:last], came[stage].at[side]
        if slot is not None:
            src, dst = part.at[side, slot], came[stage].at[side, slot - first]
        in_name = (name, stage, 0)
        if rows is not None:
            src, dst = src.at[:, rows], dst.at[:, rows]
            in_name = (name, stage, rows.start)
        send(src, dst, peer, name[0], in_name)

    def start(name, part, came, stage):
        for side in range(2):
            start_side(name, part, came, stage, side)

    def add(name, part, came, stage):
        arrived((name, stage, 0), came[stage])
        count = chips >> (stage + 1)
        for side in range(2):

            def one(slot, unused):
                total = part[side, slot].astype(full) + came[stage][side, slot].astype(full)
                part[side, slot] = total.astype(low)
                return unused

            lax.fori_loop(0, count, one, 0)

    def advance(name, part, came, split=1):
        for stage in range(stages - 1):
            add(name, part, came, stage)
            if stage < stages - 2 or split == 1:
                start(name, part, came, stage + 1)
                continue
            step = part.shape[2] // split
            for i in range(split):
                for side in range(2):
                    rows = slice(i * step, (i + 1) * step)
                    start_side(name, part, came, stage + 1, side, rows=rows)

    def choose(source, block_index, row, owner):
        rows = None
        for s in range(dp_count):
            cols = source[:, pl.ds(pl.multiple_of(block_index * block + s * strip, strip), strip)]
            rows = cols if rows is None else lax.select(owner_map[row, s] == owner, cols, rows)
        return rows

    def flip_strips(source, block_index, row):
        for r in range(chips):
            owner = relatives[r] * 2 + core
            span = max(strip, 128)
            rows = None
            for start_at in range(0, block, span):
                cols = source[:, pl.ds(pl.multiple_of(block_index * block + start_at, span), span)]
                held = owner_map[row, start_at // strip]
                for inner in range(1, span // strip):
                    held = jnp.where(owner_map[row, start_at // strip + inner] == owner, owner, held)
                rows = cols if rows is None else lax.select(held == owner, cols, rows)
            rows = rows.T
            for inner in range(span // strip):
                part = rows[inner * strip : (inner + 1) * strip]
                if inner == 0:
                    chosen = part
                    continue
                here = jnp.int32(0)
                for s in range(inner, dp_count, span // strip):
                    here = here + jnp.where(owner_map[row, s] == owner, jnp.int32(1), jnp.int32(0))
                chosen = lax.select(here == 1, part, chosen)
            flipped[0, r * strip : (r + 1) * strip, :] = chosen

    def turn(first, *chosen):
        per_block = half // width
        for r in chosen:
            q = relatives[r]
            rows = pl.ds(pl.multiple_of(lax.div(q, jnp.int32(per_block)) * block, block), block)
            inner = pl.ds(pl.multiple_of(lax.rem(q, jnp.int32(per_block)) * width, width), width)
            turned[first : first + own, pl.ds(pl.multiple_of(q * width, width), width)] = jnp.dot(
                grads2[first : first + own, rows], g_cols[rows, inner], preferred_element_type=full
            ).astype(low)

    with jax.named_scope("turn_own"):
        load_grads.wait()
        for copy in load_cols:
            copy.wait()
        turn(0, chips - 1)

    def flip(k, side, first, last):
        def one(v, unused):
            cols = pl.ds(pl.multiple_of(k * block + side * half + v * 128, 128), 128)
            rows = pl.ds(pl.multiple_of(v * 128, 128), 128)
            flipped[side, rows, first:last] = acts2[first:last, cols].T
            return unused

        lax.fori_loop(0, half // 128, one, 0)

    with jax.named_scope("flip_own"):
        load_acts.wait()
        for side in range(2):
            flip(0, side, 0, own)
    with jax.named_scope("turn_other"):
        arrived("grads", grads2.at[own:])
        turn(own, chips - 1)
    with jax.named_scope("pass_on"):
        swap_acts(2, 2 * na)
        for stage in range(1, stages):
            for relative in range(1, 1 << stage):
                pass_on(stage, relative)
        send(a_inverse, a_all.at[rows_of(chip, core)], partner, "cross", "cross")

    def multiply(k):
        part = grad_part.at[k]
        came = [came.at[k] for came in grad_came]

        def product(side, slot):
            q = chip_at(chip, slot, orders[side])
            cols = pl.ds(pl.multiple_of(q * width, width), width)
            part[side, slot] = jnp.dot(
                flipped[side], turned[:, cols], preferred_element_type=full
            ).astype(low)

        def products(side, first, last):
            def one(slot, unused):
                product(side, slot)
                return unused

            lax.fori_loop(first, last, one, 0)

        if k == 0:
            for slot in range(chips - 1, chips // 2 - 1, -1):
                if slot == chips - 2:
                    for tokens_at in (0, own):
                        turn(tokens_at, *range(chips - 1))
                for side in range(2):
                    if slot == chips - 1:
                        arrived(("acts", True, side), acts2.at[own:, side * half : (side + 1) * half])
                        flip(k, side, own, 2 * own)
                    product(side, slot)
                    start_side(("grad", k), part, came, 0, side, slot)
        else:
            for side in range(2):
                flip(k, side, 0, 2 * own)
                products(side, chips // 2, chips)
                start_side(("grad", k), part, came, 0, side)
        for side in range(2):
            products(side, 0, chips // 2)

    def advance_grad(k):
        split = 2 if k == na - 1 and stages > 1 else 1
        advance(("grad", k), grad_part.at[k], [came.at[k] for came in grad_came], split)

    def a_block(k, unused):
        flip_strips(acts2, k, k)
        for side in range(2):
            cols = pl.ds(pl.multiple_of(k * block + side * half, half), half)
            wide[...] = jnp.dot(flipped[0], acts2[:, cols], preferred_element_type=full)
            for r in range(chips):
                rows = wide[pl.ds(pl.multiple_of(r * strip + mp * sub, sub), sub), :]
                a_part[side, slot_of(r, orders[side]), k] = (rows / tokens).astype(low)
        return unused

    with jax.named_scope("multiply0"):
        multiply(0)

    with jax.named_scope("climb"):
        for r in range(1, chips):
            for side in range(2):
                climb(side, r)

    def g_block(j, unused):
        flip_strips(grads2, j, na + j)
        for side in range(2):
            cols = pl.ds(pl.multiple_of(j * block + side * half, half), half)
            wide[...] = jnp.dot(flipped[0], grads2[:, cols], preferred_element_type=full)
            for r in range(chips):
                rows = wide[r * strip : (r + 1) * strip, :]
                g_part[side, slot_of(r, orders[side]), j] = rows.astype(low)
        return unused

    def start_g():
        if not folded:
            lax.fori_loop(0, ng, g_block, 0)
            start(("g",), g_part, g_came, 0)
            return
        pick, tile, tile_came, tile_last, fold = sym

        def pick_strip(i, unused):
            r, other = lax.div(i, jnp.int32(2)), lax.rem(i, jnp.int32(2))
            owner = chip_at(chip, r, bits[::-1]) * 2 + other
            rows = choose(grads2, core, na + core, owner)
            at = pl.ds(pl.multiple_of(i * strip, strip), strip)
            pick[:, at] = rows
            flipped[lax.div(i, jnp.int32(dp_count // 2)), pl.ds(
                pl.multiple_of(lax.rem(i, jnp.int32(dp_count // 2)) * strip, strip), strip
            ), :] = rows.T
            return unused

        lax.fori_loop(0, dp_count, pick_strip, 0)

        def product(r, first, count, s, col=0, cols=2):
            at = (r % 2) * 2 * strip + first
            lhs = flipped[r // 2, at : at + count, :]
            rhs = pick[:, (s * 2 + col) * strip : (s * 2 + col + cols) * strip]
            return jnp.dot(lhs, rhs, preferred_element_type=full).astype(low)

        def slot_tiles(r, side):
            at = starts[slot_of(r, orders[side])]
            if side == 0:
                value = product(r, 0, strip, r)
                tile[side, at : at + strip] = value[:, :strip]
                tile[side, at + strip : at + nook] = value[: strip // 2, strip:]
            else:
                tile[side, at : at + nook] = product(r, strip // 2, nook, r, 1, 1)
            value = product(r, side * strip, strip, r ^ 3)
            for c in range(2):
                first = at + nook + c * strip
                tile[side, first : first + strip] = value[:, c * strip : (c + 1) * strip]

        def pair_tile(r, s, side, at):
            value = product(r, 0, 2 * strip, s)
            for c in range(2):
                first = at + c * 2 * strip
                tile[side, first : first + 2 * strip] = value[:, c * strip : (c + 1) * strip]

        for upper in (True, False):
            for side in range(2):
                near, far = 1 << orders[side][0], 1 << orders[side][1]
                for r in range(chips):
                    if (slot_of(r, orders[side]) >= chips // 2) == upper:
                        slot_tiles(r, side)
                if upper:
                    pair_tile(near, 3, side, starts[5])
                    peer = (relatives[near] * 2 + core, mp)
                    send(tile.at[side, starts[2] :], tile_came.at[side], peer, "g", "tile0")
                else:
                    pair_tile(0, far, side, starts[4])

    def advance_g():
        if not folded:
            advance(("g",), g_part, g_came)
            return
        pick, tile, tile_came, tile_last, fold = sym
        arrived("tile0", tile_came)
        for side in range(2):

            def one(i, unused):
                rows = pl.ds(pl.multiple_of(i * strip, strip), strip)
                total = tile[side, rows].astype(full) + tile_came[side, rows].astype(full)
                tile[side, rows] = total.astype(low)
                return unused

            lax.fori_loop(0, starts[2] // strip, one, 0)
            peer = (relatives[1 << orders[side][1]] * 2 + core, mp)
            send(tile.at[side, starts[1] : starts[2]], tile_last.at[side], peer, "g", "tile1")

    def finish_g():
        if not folded:
            arrived((("g",), stages - 1, 0), g_came[-1])
            for side in range(2):
                total = g_part[side, 0].astype(full) + g_came[-1][side, 0].astype(full)
                g_rows[:ng, :, side * half : (side + 1) * half] = total.astype(low)
            return
        pick, tile, tile_came, tile_last, fold = sym
        own_tiles = []
        arrived("tile1", tile_last)
        for side in range(2):

            def whole_tile(ref, at):
                parts = [ref[side, at + c * 2 * strip : at + (c + 1) * 2 * strip] for c in range(2)]
                return jnp.concatenate([part.astype(full) for part in parts], axis=1)

            fold[side] = whole_tile(tile, starts[4]) + whole_tile(tile_last, starts[1]).T
            total = tile[side, : starts[1]].astype(full) + tile_last[side, : starts[1]].astype(full)
            own_tiles.append(total[:nook])
            for c in range(2):
                first = nook + c * strip
                fold[3, side * strip : (side + 1) * strip, c * strip : (c + 1) * strip] = total[
                    first : first + strip
                ]
        cross = jnp.concatenate([own_tiles[0][strip:], own_tiles[1][: strip // 2]], axis=0)
        fold[2, :strip, :strip] = own_tiles[0][:strip]
        fold[2, :strip, strip:] = cross
        fold[2, strip:, :strip] = cross.T
        fold[2, strip:, strip:] = own_tiles[1][strip // 2 :]
        for mine, other in ((1, 1 - core), (0, core)):
            rows = pl.ds(pl.multiple_of(other * strip, strip), strip)
            for s in range(dp_count):
                found = None
                for r, place in enumerate((2, 1, 0, 3)):
                    for c in range(2):
                        value = fold[place, rows, c * strip : (c + 1) * strip]
                        here = owner_map[na + core, s] == relatives[r] * 2 + c
                        found = value if found is None else lax.select(here, value, found)
                g_rows[mine, :, s * strip : (s + 1) * strip] = found.astype(low)
            if mine:
                send(g_rows.at[1], g_rows.at[2], partner, "rows", "rows")

    for k in range(1, na):
        with jax.named_scope(f"multiply{k}"):
            if k == 1:
                arrived(("acts", False, 1), acts2.at[own:, block : 2 * block])
            multiply(k)
        if k == 1:
            with jax.named_scope("a_block"):
                load_map.wait()
                if na > 2:
                    arrived(("acts", False, 2), acts2.at[own:, 2 * block :])
                lax.fori_loop(0, na, a_block, 0)
                start(("a",), a_part, a_came, 0)
            with jax.named_scope("advance0"):
                advance_grad(0)
            with jax.named_scope("start_g"):
                start_g()
            with jax.named_scope("advance_a"):
                advance(("a",), a_part, a_came)
        else:
            with jax.named_scope(f"advance{k - 1}"):
                advance_grad(k - 1)

    with jax.named_scope("advance_g"):
        advance_g()
    with jax.named_scope("gather_a"):
        arrived((("a",), stages - 1, 0), a_came[-1])
        for side in range(2):
            total = a_part[side, 0].astype(full) + a_came[-1][side, 0].astype(full)
            a_rows[mp, :, :, side * half : (side + 1) * half] = total.astype(low)
        for m in above[1:]:
            send(a_rows.at[mp], a_rows.at[mp], (dp, m), "gather", "gather")

    climbing = a_all.at[: (chips - 1) * shard, : (mp_count - 1) * piece]
    with jax.named_scope("cross"):
        arrived("climb", climbing)
        for r in range(1, chips):
            where = a_all.at[rows_of(relatives[r], core)]
            send(where, where, partner, "cross", "cross")
    with jax.named_scope(f"advance{na - 1}"):
        advance_grad(na - 1)
    with jax.named_scope("wait_cross"):
        arrived("cross", a_all.at[: chips * shard])

    def finish(k, piece_index=0, count=1):
        step = half // count
        spans = []
        name = (("grad", k), stages - 1, piece_index * step)
        rows = slice(piece_index * step, (piece_index + 1) * step)
        arrived(name, grad_came[-1].at[k, :, :, rows])
        for side in range(2):
            total = (
                grad_part[k, side, 0, rows].astype(full) + grad_came[-1][k, side, 0, rows].astype(full)
            )
            spans.append(slice(side * half + rows.start, side * half + rows.stop))
            right[spans[-1], :] = total.astype(low)
        if piece_index:
            return
        if count == 1:
            spans = [slice(0, block)]

        def rows_done(t, unused):
            rows = pl.ds(pl.multiple_of(k * block + t * 256, 256), 256)
            inner = pl.ds(pl.multiple_of(t * 256, 256), 256)
            total = sum(
                jnp.dot(a_all[rows, span], right[span, :], preferred_element_type=full)
                for span in spans
            )
            if count > 1:
                sofar[inner, :] = total
                a_last[inner, :] = a_all[rows, :]
            else:
                out_tile[rows, :] = total.astype(low)
            return unused

        lax.fori_loop(0, block // 256, rows_done, 0)

    for k in range(na - 1):
        finish(k)
    with jax.named_scope("finish_g"):
        finish_g()
        load_old_g.wait()

        def renew(j, rows):
            g_new[j] = decay_rate * g_old[j] + (1.0 - decay_rate) * rows.astype(full)

        if folded:
            renew(core, g_rows[0])
            arrived("rows", g_rows.at[2])
            renew(1 - core, g_rows[2])
        else:
            for j in range(ng):
                renew(j, g_rows[j])
    with jax.named_scope("wait_gather"):
        arrived("gather", a_rows.at[: mp_count - 1])
    with jax.named_scope("finish_a"):
        load_old_a.wait()
        for m in range(mp_count):
            rows = slice(m * sub, (m + 1) * sub)
            a_new[:, rows, :] = decay_rate * a_old[:, rows, :] + (1.0 - decay_rate) * a_rows[m].astype(full)
    with jax.named_scope("finish_first"):
        finish(na - 1, 0, 2)
    with jax.named_scope("finish_last"):
        finish(na - 1, 1, 2)
    with jax.named_scope("drain"):
        left("grads", grads2.at[own:])
        left("acts", acts2.at[own:])
        left("spread", a_all.at[: (chips - 1) * shard, :piece])
        left("climb", climbing)
        left("cross", a_all.at[: chips * shard])
        left("grad", grad_part.at[:, :, : chips - 1])
        left("a", a_part.at[:, : chips - 1])
        if folded:
            left("g", sym[1].at[:, : 2 * starts[2] - starts[1]])
            left("rows", g_rows.at[1])
        else:
            left("g", g_part.at[:, : chips - 1])
        left("gather", a_rows.at[: mp_count - 1])


def store(first, a_new, g_new, sofar, a_last, right, out, a_out, g_out, last, sem):
    copies = [
        pltpu.make_async_copy(a_new, a_out, sem.at[0]),
        pltpu.make_async_copy(g_new, g_out, sem.at[1]),
        pltpu.make_async_copy(first, out.at[: first.shape[0]], sem.at[2]),
    ]
    for copy in copies:
        copy.start()
    block = a_last.shape[0]
    quarter = block // 4

    def one(t, unused):
        rows = pl.ds(pl.multiple_of(t * 256, 256), 256)
        total = sofar[rows, :]
        for begin in (quarter, 3 * quarter):
            span = slice(begin, begin + quarter)
            total += jnp.dot(a_last[rows, span], right[span, :], preferred_element_type=full)
        last[rows, :] = total.astype(low)
        return unused

    lax.fori_loop(0, block // 256, one, 0)
    copies.append(pltpu.make_async_copy(last, out.at[first.shape[0] :], sem.at[3]))
    copies[-1].start()
    for copy in copies:
        copy.wait()


def per_device(acts, grads_out, old_a, old_g, a_inverse, g_inverse, owner_map):
    dp_count = lax.axis_size("dp")
    mp_count = lax.axis_size("mp")
    chips = dp_count // 2
    stages = chips.bit_length() - 1
    own, features = acts.shape
    hidden = grads_out.shape[1]
    block = a_inverse.shape[1]
    na, ng = features // block, hidden // block
    strip = block // dp_count
    sub = strip // mp_count
    width = hidden // dp_count
    half = block // 2
    names_out = 10
    names_in = 9 + 2 * (chips - 1) + (na + 2) * stages + 1
    loads = 6 + block // width // 2

    def came(*shape):
        return [pltpu.VMEM((*shape[0], chips >> (s + 1), *shape[1]), low) for s in range(stages)]

    scratch = [
        pltpu.VMEM((2 * own, features), low),
        pltpu.VMEM((2 * own, hidden), low),
        pltpu.VMEM((hidden, half), low),
        pltpu.VMEM((2 * own, hidden // 2), low),
        pltpu.VMEM((features, block), low),
        pltpu.VMEM((2, half, 2 * own), low),
        pltpu.VMEM((half, half), full),
        pltpu.VMEM((mp_count, na, sub, block), low),
        pltpu.VMEM((max(ng, 3), strip, block), low),
        pltpu.VMEM((na, strip, block), full),
        pltpu.VMEM((ng, strip, block), full),
        pltpu.SMEM((na + ng, dp_count), jnp.int32),
        pltpu.VMEM((na, 2, chips, half, width), low),
        pltpu.VMEM((2, chips, ng, strip, half), low),
        pltpu.VMEM((2, chips, na, sub, half), low),
        came((na, 2), (half, width)),
        came((2,), (ng, strip, half)),
        came((2,), (na, sub, half)),
        [
            pltpu.VMEM((2 * own, block), low),
            pltpu.VMEM((2, 22 * strip, strip), low),
            pltpu.VMEM((2, 11 * strip, strip), low),
            pltpu.VMEM((2, 15 * strip // 2, strip), low),
            pltpu.VMEM((4, 2 * strip, 2 * strip), full),
        ],
        pltpu.SemaphoreType.DMA((loads,)),
        pltpu.SemaphoreType.DMA((names_out,)),
        pltpu.SemaphoreType.DMA((names_in,)),
    ]
    outside = pl.BlockSpec(memory_space=pltpu.HBM)
    results = pl.pallas_call(
        functools.partial(kernel, (dp_count, mp_count, own * dp_count)),
        out_shape=(
            pltpu.VMEM((features - block, width), low),
            pltpu.VMEM((na, strip, block), full),
            pltpu.VMEM((ng, strip, block), full),
            pltpu.VMEM((block, width), full),
            pltpu.VMEM((block, block), low),
            pltpu.VMEM((block, width), low),
        ),
        in_specs=[outside] * 7,
        out_specs=(pl.BlockSpec(memory_space=pltpu.VMEM),) * 6,
        scratch_shapes=scratch,
        compiler_params=pltpu.CompilerParams(
            collective_id=0, has_side_effects=True, vmem_limit_bytes=57 * 1024 * 1024 - 300 * 1024
        ),
        name="step",
    )(owner_map, acts, grads_out, a_inverse, g_inverse, old_a, old_g)
    out, a_new, g_new = pl.pallas_call(
        store,
        out_shape=(
            jax.ShapeDtypeStruct((features, width), low),
            jax.ShapeDtypeStruct((na, strip, block), full),
            jax.ShapeDtypeStruct((ng, strip, block), full),
        ),
        in_specs=[pl.BlockSpec(memory_space=pltpu.VMEM)] * 6,
        out_specs=(pl.BlockSpec(memory_space=pl.ANY),) * 3,
        scratch_shapes=[pltpu.VMEM((block, width), low), pltpu.SemaphoreType.DMA((4,))],
        compiler_params=pltpu.CompilerParams(vmem_limit_bytes=8 * 1024 * 1024),
        name="store",
    )(*results)
    return (a_new.reshape(old_a.shape), g_new.reshape(old_g.shape), out.reshape(features, 1, width))


def solution(mesh):
    placed = (
        P("dp", None),
        P("dp", "mp"),
        P("dp", None, None, None),
        P("mp", "dp", None, None, None),
        P("dp", None),
        P("mp", None),
        P(),
    )
    return jax.shard_map(
        per_device,
        mesh=mesh,
        in_specs=placed,
        out_specs=(P("dp", None, None, None), P("mp", "dp", None, None, None), P(None, "mp", "dp")),
        check_vma=False,
    )
```
